128 devices in a mesh: gx: 8 (over x, y_hi), gy: 16 (over y_lo, z, core).
Axes of the slice: x: 4, y: 4 (y_hi: 2, y_lo: 2; y = y_hi * 2 + y_lo), z: 4, core: 2. Of those that a mesh axis runs over, the one named last changes fastest.
Arguments:
- species: float32 [24, 128, 256, 128], P(None, 'gx', 'gy'), may hold values from -6 to 6
- diffusivity: float32 [128, 256, 128], P('gx', 'gy'), may hold values from 0.5 to 2
- lewis_number: float32 [24], replicated, may hold values from 0.5 to 2
- velocity: float32 [3, 128, 256, 128], P(None, 'gx', 'gy'), may hold values from -6 to 6
- layer_one: bfloat16 [1600, 24], replicated, may hold values from -1.25 to 1.25
- layer_two: bfloat16 [800, 1600], replicated, may hold values from -0.15625 to 0.15625
- layer_three: bfloat16 [400, 800], replicated, may hold values from -0.21875 to 0.21875
- layer_four: bfloat16 [24, 400], replicated, may hold values from -0.3125 to 0.3125
- heat_release: float32 [24], replicated, may hold values from -3 to 3
- react_index: int32 [8, 16, 4096], P('gx', 'gy'), may hold values from 0 to 32767, as said below
- react_count: int32 [8, 16], P('gx', 'gy'), may hold values from 1 to 4096, as said below
Outputs:
- species_out: float32 [24, 128, 256, 128], P(None, 'gx', 'gy')
- velocity_out: float32 [3, 128, 256, 128], P(None, 'gx', 'gy')
The draws below stay inside these ranges and needn't reach their ends.
Inputs may be any that keep to these rules, and one draw needn't show every extreme that they name: `react_index`: within each device's list the 4096 numbers are distinct cells of that device; slots from react_count on are padding. `react_count`: in every row of devices along gy the counts rounded up to whole blocks of 128 add up to at most 128, exactly that in some row; every such row has a device whose list is full.
All inputs are finite; a program needn't handle non-finite values.
Results may differ from the reference program's by a relative error of at most 0.00053.
Values may be sent and summed in bfloat16 or wider, within the bound.
A program may use at most 128 MiB of HBM per device.

```python
import math
import jax
import jax.numpy as jnp
from jax import lax

S = 24
H1 = 1600
H2 = 800
H3 = 400
CX = 16
CY = 16
NZ = 128
SUBSTEPS = 2
BLOCK = 128
BWORK = 8
BCAP = 32
RCAP = 4096
CELLS_DEV = 32768
NX = 128
NY = 256
GROUPS_X = 8
GROUPS_Y = 16


def draw_velocity(key, part):
    noise = jnp.clip(jax.random.normal(jax.random.fold_in(key, 21), (3, NX, NY, NZ), jnp.float32), -4.0, 4.0)
    return noise


def draw_react_index(key, part):
    keys = jax.random.split(jax.random.fold_in(key, 11), GROUPS_X * GROUPS_Y)

    def one_list(single):
        return jax.random.permutation(single, CELLS_DEV)[:RCAP]
    lists = jax.vmap(one_list)(keys)
    return lists.reshape(GROUPS_X, GROUPS_Y, RCAP).astype(jnp.int32)


def draw_react_count(key, part):
    most = GROUPS_Y * BWORK
    drops = jax.random.randint(jax.random.fold_in(key, 1), (GROUPS_X,), 0, most // 4 + 1)
    fullest = jax.random.randint(jax.random.fold_in(key, 2), (), 0, GROUPS_X)
    drops = jnp.where(jnp.arange(GROUPS_X) == fullest, 0, drops)
    target = most - drops
    chosen = jax.random.randint(jax.random.fold_in(key, 3), (GROUPS_X,), 0, GROUPS_Y)
    places = jnp.arange(GROUPS_Y)
    is_chosen = places[None, :] == chosen[:, None]
    weights = jax.random.randint(jax.random.fold_in(key, 4), (GROUPS_X, GROUPS_Y), 1, 8)
    weights = jnp.where(is_chosen, 0, weights)
    remain = target - BCAP - (GROUPS_Y - 1)
    shares = remain[:, None] * weights // jnp.sum(weights, axis=1)[:, None]
    leftover = remain - jnp.sum(shares, axis=1)
    ordinal = places[None, :] - (places[None, :] > chosen[:, None]).astype(jnp.int32)
    extra = ((ordinal < leftover[:, None]) & jnp.logical_not(is_chosen)).astype(jnp.int32)
    blocks = jnp.where(is_chosen, BCAP, 1 + shares + extra)
    tails = jax.random.randint(jax.random.fold_in(key, 5), (GROUPS_X, GROUPS_Y), 1, BLOCK + 1)
    counts = jnp.where(is_chosen, BCAP * BLOCK, (blocks - 1) * BLOCK + tails)
    return counts.astype(jnp.int32)


def block_levels(rng, shape, pieces, low, largest):
    def one(axis_at, parts):
        draws = jax.random.uniform(jax.random.fold_in(jax.random.fold_in(rng, 6), axis_at), (parts,), jnp.float32, low / len(pieces), largest / len(pieces))
        return jnp.repeat(jnp.exp(draws), shape[axis_at] // parts).reshape((-1,) + (1,) * (len(shape) - axis_at - 1))

    factor_of = one(*pieces[0])
    for cut in pieces[1:]:
        factor_of = factor_of * one(*cut)
    return factor_of


def gaussian(stream_key, extent, scale, reach, cuts=(), held_as=jnp.bfloat16):
    entries = jax.random.normal(stream_key, extent, jnp.float32) * scale
    if len(cuts) > 0:
        entries = block_levels(stream_key, extent, cuts, -0.22, 0.18) * entries
    return jnp.clip(entries, min=-reach, max=reach).astype(held_as)


def setup_inputs(seed: int = 0) -> dict:
    key_list = jax.random.split(jax.random.key(seed), 12)
    species = gaussian(key_list[0], (S, NX, NY, NZ), 1.0, 6.0, ((1, 8), (2, 16)), jnp.float32)
    diffusivity = jnp.clip(jnp.exp(math.log(2.0) - 1.3862944 * jax.random.uniform(key_list[1], (NX, NY, NZ), jnp.float32) ** block_levels(key_list[1], (NX, NY, NZ), ((0, 8), (1, 16)), -0.2, 0.2)), 0.5, 2.0)
    lewis_number = jnp.clip(jnp.exp(jax.random.uniform(key_list[2], (S,), jnp.float32, math.log(0.5), math.log(2.0))), 0.5, 2.0)
    velocity = draw_velocity(jax.random.fold_in(key_list[11], 71), 0)
    layer_one = gaussian(key_list[4], (H1, S), S ** -0.5, 1.25)
    layer_two = gaussian(key_list[5], (H2, H1), H1 ** -0.5, 0.15625)
    layer_three = gaussian(key_list[6], (H3, H2), H2 ** -0.5, 0.21875)
    layer_four = gaussian(key_list[7], (S, H3), H3 ** -0.5, 0.3125)
    heat_release = gaussian(key_list[8], (S,), 0.5, 3.0, (), jnp.float32)
    react_index = draw_react_index(jax.random.fold_in(key_list[11], 71), 0)
    react_count = draw_react_count(jax.random.fold_in(key_list[11], 71), 0)
    return dict(species=species, diffusivity=diffusivity, lewis_number=lewis_number, velocity=velocity, layer_one=layer_one, layer_two=layer_two, layer_three=layer_three, layer_four=layer_four, heat_release=heat_release, react_index=react_index, react_count=react_count)


diffuse_step = 0.03
react_step = 0.5


def diffuse_whole(values, coeffs):
    terms = []
    for axis in range(3):
        after = jnp.roll(values, -1, axis)
        before = jnp.roll(values, 1, axis)
        coef_after = jnp.roll(coeffs, -1, axis)
        coef_before = jnp.roll(coeffs, 1, axis)
        upward = 0.5 * (coeffs + coef_after) * (after - values)
        downward = 0.5 * (coef_before + coeffs) * (values - before)
        terms.append(upward - downward)
    return values + diffuse_step * ((terms[0] + terms[1]) + terms[2])


def network_rows(rows, first, second, third, fourth):
    hidden = jax.nn.silu(jnp.dot(rows, first.T, preferred_element_type=jnp.float32)).astype(jnp.bfloat16)
    hidden = jax.nn.silu(jnp.dot(hidden, second.T, preferred_element_type=jnp.float32)).astype(jnp.bfloat16)
    hidden = jax.nn.silu(jnp.dot(hidden, third.T, preferred_element_type=jnp.float32)).astype(jnp.bfloat16)
    return jnp.dot(hidden, fourth.T, preferred_element_type=jnp.float32).astype(jnp.bfloat16)


def inverse_symbol(wave_x, wave_y, wave_z, size_x, size_y, size_z):
    along_x = 2.0 * jnp.cos(wave_x.astype(jnp.float32) * (2.0 * jnp.pi / size_x)) - 2.0
    along_y = 2.0 * jnp.cos(wave_y.astype(jnp.float32) * (2.0 * jnp.pi / size_y)) - 2.0
    along_z = 2.0 * jnp.cos(wave_z.astype(jnp.float32) * (2.0 * jnp.pi / size_z)) - 2.0
    symbol = along_x[:, None, None] + along_y[None, :, None] + along_z[None, None, :]
    anchor = (wave_x[:, None, None] == 0) & (wave_y[None, :, None] == 0) & (wave_z[None, None, :] == 0)
    return jnp.where(anchor, 0.0, 1.0 / jnp.where(anchor, 1.0, symbol))


def reference(species, diffusivity, lewis_number, velocity, layer_one, layer_two, layer_three, layer_four, heat_release, react_index, react_count):
    def one_species(packed):
        values, lewis = packed
        coeffs = diffusivity / lewis
        for substep in range(SUBSTEPS):
            values = diffuse_whole(values, coeffs)
        return values

    diffused = lax.map(one_species, (species, lewis_number))
    flat_fields = diffused.reshape(S, NX * NY * NZ)

    live_blocks = ((react_count + BLOCK - 1) // BLOCK).astype(jnp.int32)
    starts = (jnp.cumsum(live_blocks, axis=1) - live_blocks).astype(jnp.int32)
    slot_ids = jnp.arange(GROUPS_Y * BWORK, dtype=jnp.int32)
    row_ids = jnp.arange(BLOCK, dtype=jnp.int32)

    def group_rows(packed):
        starts_row, live_row, counts_row, index_rows, column = packed
        owner = jnp.sum((starts_row[None, :] <= slot_ids[:, None]).astype(jnp.int32), axis=1) - 1
        block = slot_ids - starts_row[owner]
        valid = block < live_row[owner]
        block = jnp.where(valid, block, 0).astype(jnp.int32)
        position = (block[:, None] * BLOCK + row_ids[None, :]).astype(jnp.int32)
        local = index_rows[owner[:, None], position]
        living = valid[:, None] & (position < counts_row[owner][:, None])
        cell_x = column * CX + local // (CY * NZ)
        cell_y = owner[:, None] * CY + (local // NZ) % CY
        cell_z = local % NZ
        global_ids = ((cell_x * NY + cell_y) * NZ + cell_z).astype(jnp.int32).reshape(-1)
        rows = flat_fields[:, global_ids].T.astype(jnp.bfloat16)
        rate_rows = network_rows(rows, layer_one, layer_two, layer_three, layer_four)
        return global_ids, living.reshape(-1), rate_rows

    columns = jnp.arange(GROUPS_X, dtype=jnp.int32)
    global_ids, living, rate_rows = lax.map(group_rows, (starts, live_blocks, react_count, react_index, columns))
    global_ids = global_ids.reshape(-1)
    living = living.reshape(-1)
    rate_rows = rate_rows.reshape(-1, S).astype(jnp.float32)
    update = jnp.where(living[:, None], react_step * rate_rows, 0.0)
    species_out = flat_fields.at[:, global_ids].add(update.T).reshape(S, NX, NY, NZ)
    heat_rows = jnp.where(living, jnp.dot(rate_rows, heat_release, precision=lax.Precision.HIGHEST), 0.0)
    heat = jnp.zeros((NX * NY * NZ,), jnp.float32).at[global_ids].add(heat_rows).reshape(NX, NY, NZ)

    divergence = (jnp.roll(velocity[0], -1, 0) - velocity[0]) + (jnp.roll(velocity[1], -1, 1) - velocity[1]) + (jnp.roll(velocity[2], -1, 2) - velocity[2])
    source = divergence - heat
    symbol = inverse_symbol(jnp.arange(NX, dtype=jnp.int32), jnp.arange(NY, dtype=jnp.int32), jnp.arange(NZ, dtype=jnp.int32), NX, NY, NZ)
    pressure = jnp.real(jnp.fft.ifftn(jnp.fft.fftn(source) * symbol)).astype(species.dtype)
    gradient = jnp.stack([pressure - jnp.roll(pressure, 1, 0), pressure - jnp.roll(pressure, 1, 1), pressure - jnp.roll(pressure, 1, 2)])
    velocity_out = velocity - gradient
    return species_out, velocity_out
```

```python
import functools
import numpy as np
import jax
import jax.numpy as jnp
from jax import lax
from jax.experimental import pallas as pl
from jax.experimental.pallas import tpu as pltpu

from jax.sharding import PartitionSpec as P

MESH = pl.DeviceIdType.MESH
HI = lax.Precision.HIGHEST


def real_basis(n):
    k = np.arange(n)
    j = np.arange(n)
    wave = np.where(k <= n // 2, k, k - n // 2)
    ang = 2.0 * np.pi * ((wave[:, None] * j[None, :]) % n) / n
    rows = np.where((k <= n // 2)[:, None], np.cos(ang), np.sin(ang)) * np.sqrt(2.0 / n)
    rows[0] *= np.sqrt(0.5)
    rows[n // 2] *= np.sqrt(0.5)
    lam = 2.0 * np.cos(2.0 * np.pi * wave / n) - 2.0
    return rows.astype(np.float32), lam.astype(np.float32)


def mm(a, b, dims, precision=HI):
    return lax.dot_general(a, b, (dims, ((), ())), precision=precision, preferred_element_type=jnp.float32)


def units(grid, lane):
    turned = []
    for d in range(8):
        w = grid[d]
        for u in range(1, 8):
            w = jnp.where(lane == u, grid[(u + d) % 8], w)
        turned.append(w if d == 0 else pltpu.roll(w, d * 16, 1))
    out = []
    for v in range(8):
        acc = turned[(0 - v) % 8]
        for u in range(1, 8):
            acc = jnp.where(lane == u, turned[(u - v) % 8], acc)
        out.append(acc)
    return out


def poisson_kernel(gx_n, gy_n, src, vel, fz, fx, fxt, fy, lamx, lamy, lamz, out,
                   sbuf, rbuf, tbuf, pbuf, send_sem, recv_sem, send_sem2, recv_sem2):
    gx = lax.axis_index("gx")
    gy = lax.axis_index("gy")
    n = gx_n * gy_n
    me = gx * gy_n + gy
    barrier = pltpu.get_barrier_semaphore()

    def greet(i, c):
        t = lax.rem(me + i, n)
        pl.semaphore_signal(barrier, inc=1, device_id=(t // gy_n, lax.rem(t, gy_n)), device_id_type=MESH)
        return c
    lax.fori_loop(1, n, greet, 0)
    zt = mm(fz[...], src[...], ((1,), (1,)))
    sbuf[:, 0, :] = zt[:, :128]
    sbuf[:, 1, :] = zt[:, 128:]
    pl.semaphore_wait(barrier, n - 1)

    def send(i, c):
        t = lax.rem(me + i, n)
        ta, tb = t // gy_n, lax.rem(t, gy_n)
        pltpu.make_async_remote_copy(
            src_ref=sbuf.at[t], dst_ref=rbuf.at[gy, gx], send_sem=send_sem, recv_sem=recv_sem,
            device_id=(ta, tb), device_id_type=MESH).start()
        return c
    lax.fori_loop(1, n, send, 0)
    own = pltpu.make_async_copy(sbuf.at[me], rbuf.at[gy, gx], recv_sem)
    own.start()
    lane = lax.broadcasted_iota(jnp.int32, (8, 128), 1) // 16
    col = lax.broadcasted_iota(jnp.int32, (8, 128), 1)
    mode = lax.broadcasted_iota(jnp.int32, (1, 128), 1)
    lz = jnp.sum(jnp.where(mode == me, lamz[...], 0.0), axis=1, keepdims=True)
    sym = lamx[...] + lamy[...] + lz
    anchor = (lax.broadcasted_iota(jnp.int32, (128, 256), 0) == 0) & (lax.broadcasted_iota(jnp.int32, (128, 256), 1) == 0) & (me == 0)
    g = jnp.where(anchor, 0.0, 1.0 / jnp.where(anchor, 1.0, sym))
    pltpu.make_async_copy(rbuf, rbuf, recv_sem).wait()
    pltpu.make_async_copy(sbuf.at[pl.ds(0, n - 1)], sbuf.at[pl.ds(0, n - 1)], send_sem).wait()

    planes = [[None, None] for _ in range(16)]
    for h in range(2):
        for bh in range(2):
            got = units([rbuf[bh * 8 + b, :, h, :] for b in range(8)], lane)
            for xlo in range(8):
                planes[h * 8 + xlo][bh] = got[xlo]
    plane = jnp.concatenate([jnp.concatenate(p, axis=1) for p in planes], axis=0)
    t = mm(fx[...], plane, ((1,), (0,)))
    t = mm(t, fy[...], ((1,), (1,))) * g
    t = mm(t, fy[...], ((1,), (0,)))
    p = mm(fxt[...], t, ((1,), (0,)))
    px = [[p[x * 8:(x + 1) * 8, bh * 128:(bh + 1) * 128] for bh in range(2)] for x in range(16)]
    before = pltpu.roll(p, 1, 1)
    for bh in range(2):
        edge_x = pltpu.roll(px[15][bh], 1, 0)
        edge_y = before[0:8, bh * 128:(bh + 1) * 128]
        for x in range(1, 16):
            edge_y = jnp.where(col % 16 == x, pltpu.roll(before[x * 8:(x + 1) * 8, bh * 128:(bh + 1) * 128], x, 1), edge_y)
        for h in range(2):
            got = units([px[h * 8 + xlo][bh] for xlo in range(8)], lane)
            for b in range(8):
                tbuf[bh * 8 + b, :, h, :] = got[b]
        for b in range(8):
            ex = edge_x if b == 0 else pltpu.roll(edge_x, 128 - b * 16, 1)
            ey = pltpu.roll(edge_y, (128 - b * 16 + 16) % 128, 1) if b != 1 else edge_y
            tbuf[bh * 8 + b, :, 2, :] = jnp.where(lane == 0, ex, ey)

    def back(i, c):
        t = lax.rem(me + i, n)
        ta, tb = t // gy_n, lax.rem(t, gy_n)
        pltpu.make_async_remote_copy(
            src_ref=tbuf.at[tb, ta], dst_ref=pbuf.at[me], send_sem=send_sem2, recv_sem=recv_sem2,
            device_id=(ta, tb), device_id_type=MESH).start()
        return c
    lax.fori_loop(1, n, back, 0)
    own = pltpu.make_async_copy(tbuf.at[gy, gx], pbuf.at[me], recv_sem2)
    own.start()
    pltpu.make_async_copy(pbuf, pbuf, recv_sem2).wait()
    pltpu.make_async_copy(pbuf.at[pl.ds(0, n - 1)], pbuf.at[pl.ds(0, n - 1)], send_sem2).wait()
    rows = [mm(pbuf[:, h, :], fz[...], ((0,), (0,))) for h in range(3)]
    q = jnp.concatenate(rows[:2], axis=0)
    west = rows[2][0:16]
    south = rows[2][16:32]
    out[2] = vel[2] - (q - pltpu.roll(q, 1, 1))
    out[0] = vel[0] - (q - jnp.concatenate([west, q[:240]], axis=0))
    sub = lax.broadcasted_iota(jnp.int32, (16, 128), 0)
    for x in range(16):
        cur = q[x * 16:(x + 1) * 16]
        prev = jnp.where(sub == 0, jnp.broadcast_to(south[x:x + 1], (16, 128)), pltpu.roll(cur, 1, 0))
        out[1, x * 16:(x + 1) * 16] = vel[1, x * 16:(x + 1) * 16] - (cur - prev)


def poisson(source, velocity):
    gx_n, gy_n = lax.axis_size("gx"), lax.axis_size("gy")
    fz, lz = real_basis(128)
    fx, lx = real_basis(128)
    fy, ly = real_basis(256)
    fxp = fx.reshape(128, 8, 16).transpose(0, 2, 1).reshape(128, 128)
    vm = pl.BlockSpec(memory_space=pltpu.VMEM)
    args = (source.reshape(256, 128), velocity.reshape(3, 256, 128), jnp.asarray(fz), jnp.asarray(fxp), jnp.asarray(np.ascontiguousarray(fxp.T)), jnp.asarray(fy),
            jnp.asarray(lx[:, None]), jnp.asarray(ly[None, :]), jnp.asarray(lz[None, :]))
    out = pl.pallas_call(
        functools.partial(poisson_kernel, gx_n, gy_n),
        out_shape=jax.ShapeDtypeStruct((3, 256, 128), jnp.float32),
        in_specs=[vm] * len(args), out_specs=vm,
        scratch_shapes=[
            pltpu.VMEM((128, 2, 128), jnp.float32), pltpu.VMEM((16, 8, 2, 128), jnp.float32),
            pltpu.VMEM((16, 8, 3, 128), jnp.float32), pltpu.VMEM((128, 3, 128), jnp.float32),
            pltpu.SemaphoreType.DMA, pltpu.SemaphoreType.DMA, pltpu.SemaphoreType.DMA, pltpu.SemaphoreType.DMA],
        compiler_params=pltpu.CompilerParams(collective_id=1, has_side_effects=True),
        name="poisson",
    )(*args)
    return out.reshape(velocity.shape)


SUBSTEPS = 2
BLOCK = 128


diffuse_step = 0.03
react_step = 0.5


def in_one_piece(arrays, axis, split_dim, concat_dim, along):
    both = jnp.concatenate(arrays, axis=along)
    filled, at, finished = (
        lax.all_to_all(both, axis, split_axis=split_dim, concat_axis=concat_dim, tiled=True),
        0,
        [],
    )
    for a in arrays:
        finished.append(lax.slice_in_dim(filled, at, at + a.shape[along], axis=along))
        at += a.shape[along]
    return tuple(finished)


def extended(value, sides, width):
    edges = {}
    for axis, dim in sides:
        peers, length = (lax.axis_size(axis), value.shape[dim])
        up = [(i, (i + 1) % peers) for i in range(peers)]
        last = lax.slice_in_dim(value, length - width, length, axis=dim)
        leading = lax.slice_in_dim(value, 0, width, axis=dim)
        edges[dim] = (
            lax.ppermute(last, axis, up),
            lax.ppermute(leading, axis, [(b, a) for a, b in up]),
        )
    done = []
    for _, dim in sides:
        low, high = edges[dim]
        around = [(width, width) if d in done else (0, 0) for d in range(value.ndim)]
        value = jnp.concatenate([jnp.pad(low, around), value, jnp.pad(high, around)], axis=dim)
        done.append(dim)
    return value


def from_behind(value, axis, by):
    peers = lax.axis_size(axis)
    return lax.ppermute(value, axis, [(i, (i + by) % peers) for i in range(peers)])


def diffuse(padded, coeffs):
    center = padded[:, 1:-1, 1:-1, :]
    middle = coeffs[:, 1:-1, 1:-1, :]
    east_flux = 0.5 * (middle + coeffs[:, 2:, 1:-1, :]) * (padded[:, 2:, 1:-1, :] - center)
    west_flux = 0.5 * (coeffs[:, :-2, 1:-1, :] + middle) * (center - padded[:, :-2, 1:-1, :])
    north_flux = 0.5 * (middle + coeffs[:, 1:-1, 2:, :]) * (padded[:, 1:-1, 2:, :] - center)
    south_flux = 0.5 * (coeffs[:, 1:-1, :-2, :] + middle) * (center - padded[:, 1:-1, :-2, :])
    upper_flux = 0.5 * (middle + jnp.roll(middle, -1, 3)) * (jnp.roll(center, -1, 3) - center)
    lower_flux = 0.5 * (jnp.roll(middle, 1, 3) + middle) * (center - jnp.roll(center, 1, 3))
    updated = center + diffuse_step * (
        east_flux - west_flux + (north_flux - south_flux) + (upper_flux - lower_flux)
    )
    return (updated, middle)


def network(blocks, first, second, third, fourth):
    hidden = jax.nn.silu(
        jnp.einsum("fs,bsr->bfr", first, blocks, preferred_element_type=jnp.float32)
    ).astype(jnp.bfloat16)
    hidden = jax.nn.silu(
        jnp.einsum("gf,bfr->bgr", second, hidden, preferred_element_type=jnp.float32)
    ).astype(jnp.bfloat16)
    hidden = jax.nn.silu(
        jnp.einsum("hg,bgr->bhr", third, hidden, preferred_element_type=jnp.float32)
    ).astype(jnp.bfloat16)
    return jnp.einsum("sh,bhr->bsr", fourth, hidden, preferred_element_type=jnp.float32).astype(
        jnp.bfloat16
    )


def per_device(
    species,
    diffusivity,
    lewis_number,
    velocity,
    layer_one,
    layer_two,
    layer_three,
    layer_four,
    heat_release,
    react_index,
    react_count,
):
    kinds = species.shape[0]
    fields = species
    for substep in range(SUBSTEPS):
        padded, kappa_pad = (
            extended(fields, (("gx", 1), ("gy", 2)), 1),
            extended(diffusivity[None], (("gx", 1), ("gy", 2)), 1),
        )
        coeffs = kappa_pad / lewis_number[:, None, None, None]
        fields, unused = diffuse(padded, coeffs)
    cells = fields.shape[1] * fields.shape[2] * fields.shape[3]
    flat = fields.reshape(kinds, cells)
    index_list = react_index.reshape(-1)
    capacity = index_list.shape[0]
    slots = capacity // BLOCK
    count_here = react_count.reshape(())
    chosen = jnp.take(flat, index_list, axis=1).astype(jnp.bfloat16)
    blocks = chosen.reshape(kinds, slots, BLOCK).transpose(1, 0, 2)
    rate_blocks = network(blocks, layer_one, layer_two, layer_three, layer_four).astype(jnp.float32)
    rate_rows = rate_blocks.transpose(1, 0, 2).reshape(kinds, capacity)
    live_mask = jnp.arange(capacity, dtype=jnp.int32) < count_here
    update = jnp.where(live_mask[None, :], react_step * rate_rows, 0.0)
    species_out = flat.at[:, index_list].add(update).reshape(fields.shape)
    heat_rows = jnp.where(
        live_mask, jnp.dot(heat_release, rate_rows, precision=lax.Precision.HIGHEST), 0.0
    )
    heat_field = (
        jnp.zeros((cells,), jnp.float32).at[index_list].add(heat_rows).reshape(fields.shape[1:])
    )
    flow_x = velocity[0]
    flow_y = velocity[1]
    flow_z = velocity[2]
    east_plane = from_behind(flow_x[0:1], "gx", -1)
    north_plane = from_behind(flow_y[:, 0:1], "gy", -1)
    divergence = (
        jnp.concatenate([flow_x[1:], east_plane], axis=0)
        - flow_x
        + (jnp.concatenate([flow_y[:, 1:], north_plane], axis=1) - flow_y)
        + (jnp.roll(flow_z, -1, 2) - flow_z)
    )
    source = divergence - heat_field
    velocity_out = poisson(source, velocity)
    return (species_out, velocity_out)


def solution(mesh):
    return jax.shard_map(
        per_device,
        mesh=mesh,
        in_specs=(
            P(None, "gx", "gy", None),
            P("gx", "gy", None),
            P(),
            P(None, "gx", "gy", None),
            P(),
            P(),
            P(),
            P(),
            P(),
            P("gx", "gy", None),
            P("gx", "gy"),
        ),
        out_specs=(P(None, "gx", "gy", None), P(None, "gx", "gy", None)),
        check_vma=False,
    )
```

```python
import functools

import jax
import jax.numpy as jnp
import numpy as np
from jax import lax
from jax.experimental import pallas as pl
from jax.experimental.pallas import tpu as pltpu
from jax.sharding import PartitionSpec as P

MESH = pl.DeviceIdType.MESH
HI = lax.Precision.HIGHEST
BF = jnp.bfloat16
PITCH = 24


def next_along(v):
    return pltpu.roll(v, 127, 1)


def transport_kernel(gx_n, gy_n, sp, dif, cs, vel, idx, fout, chem, div,
                     stage, y0, y1, dp, ax, ay, az, gb, sendx, recvx, sendy, recvy, sendc, recvc, sendv, recvv,
                     load_sem, ssem, rsem):
    gx = lax.axis_index("gx")
    gy = lax.axis_index("gy")
    east, west = lax.rem(gx + 1, gx_n), lax.rem(gx + gx_n - 1, gx_n)
    north, south = lax.rem(gy + 1, gy_n), lax.rem(gy + gy_n - 1, gy_n)
    diag = ((east, north), (east, south), (west, north), (west, south))
    barrier = pltpu.get_barrier_semaphore()
    for dev in ((east, gy), (west, gy), (gx, north), (gx, south)) + diag:
        pl.semaphore_signal(barrier, inc=1, device_id=dev, device_id_type=MESH)
    order = (14, 15, 0, 1) + tuple(range(2, 14))
    loads = {}
    for x in order:
        loads[x] = pltpu.make_async_copy(sp.at[:, x], stage.at[x], load_sem.at[x])
        loads[x].start()

    flat = stage.reshape(16 * 24 * 16, 128)

    def spread(x):
        for y in range(16):
            y0[(x + 2) * 20 + y + 2] = flat[pl.ds(x * 384 + y, 24, stride=16), :]

    def copy(src, dst, k, dev):
        return pltpu.make_async_remote_copy(src_ref=src, dst_ref=dst, send_sem=ssem.at[k], recv_sem=rsem.at[k],
                                            device_id=dev, device_id_type=MESH)

    sendv[0] = vel[0, 0:16, :]
    for x in range(16):
        sendv[1, x:x + 1, :] = vel[1, x * 16:x * 16 + 1, :]
    copies = [copy(sendx.at[0], recvx.at[0], 0, (east, gy)), copy(sendx.at[1], recvx.at[1], 1, (west, gy)),
              copy(sendy.at[0], recvy.at[0], 2, (gx, north)), copy(sendy.at[1], recvy.at[1], 3, (gx, south)),
              copy(sendc.at[0], recvc.at[0], 4, diag[0]), copy(sendc.at[1], recvc.at[1], 5, diag[1]),
              copy(sendc.at[2], recvc.at[2], 6, diag[2]), copy(sendc.at[3], recvc.at[3], 7, diag[3]),
              copy(sendv.at[0], recvv.at[0], 8, (west, gy)), copy(sendv.at[1], recvv.at[1], 9, (gx, south))]

    def at(x, y):
        return y0[(x + 2) * 20 + y + 2]

    for d, planes in ((0, (14, 15)), (1, (0, 1))):
        for p, x in enumerate(planes):
            loads[x].wait()
            spread(x)
            for y in range(0, 16, 2):
                sendx[d, p, y * 24:y * 24 + 48, :] = jnp.concatenate([at(x, y), at(x, y + 1)], axis=0).astype(BF)
            sendx[d, p, 384:400, :] = dif[x].astype(BF)
        if d == 0:
            pl.semaphore_wait(barrier, 8)
        copies[d].start()
    for x in range(2, 14):
        loads[x].wait()
        spread(x)
    for d, planes in ((0, (14, 15)), (1, (0, 1))):
        for p, y in enumerate(planes):
            for x in range(0, 16, 2):
                sendy[d, p, x * 24:x * 24 + 48, :] = jnp.concatenate([at(x, y), at(x + 1, y)], axis=0).astype(BF)
            sendy[d, p, 384:400, :] = jnp.concatenate([dif[x, y:y + 1, :] for x in range(16)], axis=0).astype(BF)
        copies[2 + d].start()
    for k, (x, y) in enumerate(((15, 15), (15, 0), (0, 15), (0, 0))):
        drow = jnp.broadcast_to(dif[x, y:y + 1, :], (8, 128))
        sendc[k] = jnp.concatenate([at(x, y), drow], axis=0).astype(BF)
        copies[4 + k].start()
    copies[8].start()
    copies[9].start()

    for x in range(16):
        dp[pl.ds((x + 2) * PITCH + 2, 16), :] = dif[x]

    def conduct():
        d = dp[...]
        ax[...] = 0.5 * (d + jnp.concatenate([d[PITCH:], d[:PITCH]], axis=0))
        ay[...] = 0.5 * (d + pltpu.roll(d, 20 * PITCH - 1, 0))
        az[...] = 0.5 * (d + next_along(d))
    conduct()
    scale = cs[...]

    def step(src, i, j):
        c = src[i * 20 + j]
        r = i * PITCH + j
        fx = ax[pl.ds(r, 1), :] * (src[i * 20 + j + 20] - c) - ax[pl.ds(r - PITCH, 1), :] * (c - src[i * 20 + j - 20])
        fy = ay[pl.ds(r, 1), :] * (src[i * 20 + j + 1] - c) - ay[pl.ds(r - 1, 1), :] * (c - src[i * 20 + j - 1])
        t = az[pl.ds(r, 1), :] * (next_along(c) - c)
        return c + scale * (fx + fy + (t - pltpu.roll(t, 1, 1)))

    def first(lo, hi, js):
        def body(i, carry):
            for j in js:
                y1[i * 20 + j] = step(y0, i, j)
            return carry
        lax.fori_loop(lo, hi, body, 0)

    def second(pair):
        def body(y, carry):
            both = [step(y1, x + 2, y + 2) for x in (pair, 15 - pair)]
            val = jnp.concatenate(both, axis=1)
            fout[pl.ds(pl.multiple_of((pair * 16 + y) * 24, 8), 24), :] = val
            return carry
        lax.fori_loop(0, 16, body, 0)

        def pack(q, carry):
            base = pl.multiple_of(pair * 384 + q * 48, 16)
            gb[pl.ds(base, 48), :] = fout[pl.ds(base, 48), :].astype(BF)
            return carry
        lax.fori_loop(0, 8, pack, 0)

    rows256 = lax.broadcasted_iota(jnp.int32, (256, 256), 0)

    def gather(pairs_lo, pairs_hi, fresh):
        def group(g, carry):
            c = idx[:, pl.ds(pl.multiple_of(g * 256, 256), 256)]
            x = c // 2048
            high = x >= 8
            xyh = jnp.where(high, 15 - x, x) * 16 + (c // 128) % 16
            kk = jnp.where(high, 128, 0) + c % 128
            pick = jnp.where(rows256 == kk, 1.0, 0.0).astype(BF)
            acc = jnp.zeros((24, 256), jnp.float32)
            for pr in range(pairs_lo, pairs_hi):
                t = jnp.dot(gb[pr * 384:(pr + 1) * 384, :], pick, preferred_element_type=jnp.float32)
                for q in range(16):
                    acc = acc + jnp.where(xyh == pr * 16 + q, t[q * 24:(q + 1) * 24], 0.0)
            where = pl.ds(pl.multiple_of(g * 256, 256), 256)
            if fresh:
                chem[:, where] = acc.astype(BF)
            else:
                chem[:, where] = (chem[:, where].astype(jnp.float32) + acc).astype(BF)
            return carry
        lax.fori_loop(0, 16, group, 0)

    first(3, 17, tuple(range(3, 17)))
    for k in (2, 3):
        copies[k].wait_recv()
    for d, js in ((0, (0, 1)), (1, (18, 19))):
        for p, j in enumerate(js):
            for x in range(0, 16, 2):
                two = recvy[d, p, x * 24:x * 24 + 48, :].astype(jnp.float32)
                y0[(x + 2) * 20 + j] = two[:24]
                y0[(x + 3) * 20 + j] = two[24:]
            drows = recvy[d, p, 384:400, :].astype(jnp.float32)
            for x in range(16):
                dp[pl.ds((x + 2) * PITCH + j, 1), :] = drows[x:x + 1]
    conduct()
    first(3, 17, (1, 2, 17, 18))
    for pair in range(2, 8):
        second(pair)
    gather(2, 8, True)
    for k in (0, 1, 4, 5, 6, 7, 8, 9):
        copies[k].wait_recv()
    for d, iis in ((0, (0, 1)), (1, (18, 19))):
        for p, i in enumerate(iis):
            for y in range(0, 16, 2):
                two = recvx[d, p, y * 24:y * 24 + 48, :].astype(jnp.float32)
                y0[i * 20 + y + 2] = two[:24]
                y0[i * 20 + y + 3] = two[24:]
            dp[pl.ds(i * PITCH + 2, 16), :] = recvx[d, p, 384:400, :].astype(jnp.float32)
    for k, (i, j) in enumerate(((1, 1), (1, 18), (18, 1), (18, 18))):
        val = recvc[k].astype(jnp.float32)
        y0[i * 20 + j] = val[:24]
        dp[pl.ds(i * PITCH + j, 1), :] = val[24:25]
    conduct()
    for i in (1, 18):
        first(i, i + 1, tuple(range(2, 18)))
    for i in (2, 17):
        first(i, i + 1, tuple(range(1, 19)))
    for pair in range(2):
        second(pair)
    gather(0, 2, False)

    ux, uy, uz = vel[0], vel[1], vel[2]
    sub = lax.broadcasted_iota(jnp.int32, (16, 128), 0)
    for x in range(16):
        here = slice(x * 16, x * 16 + 16)
        nx = recvv[0] if x == 15 else vel[0, x * 16 + 16:x * 16 + 32, :]
        uy = vel[1, here, :]
        ny = jnp.where(sub == 15, jnp.broadcast_to(recvv[1, x:x + 1, :], (16, 128)), pltpu.roll(uy, 15, 0))
        uz = vel[2, here, :]
        div[here, :] = (nx - vel[0, here, :]) + (ny - uy) + (next_along(uz) - uz)
    for c in copies:
        c.wait_send()


def transport(species, diffusivity, lewis_number, velocity, react_index):
    gx_n, gy_n = lax.axis_size("gx"), lax.axis_size("gy")
    vm = pl.BlockSpec(memory_space=pltpu.VMEM)
    hb = pl.BlockSpec(memory_space=pl.ANY)
    cs = jnp.broadcast_to((0.03 / lewis_number)[:, None], (24, 128))
    f32 = jnp.float32
    return pl.pallas_call(
        functools.partial(transport_kernel, gx_n, gy_n),
        out_shape=(jax.ShapeDtypeStruct((3072, 256), f32), jax.ShapeDtypeStruct((24, 4096), BF),
                   jax.ShapeDtypeStruct((256, 128), f32)),
        in_specs=[hb, vm, vm, vm, vm], out_specs=(vm, vm, vm),
        scratch_shapes=[
            pltpu.VMEM((16, 24, 16, 128), f32), pltpu.VMEM((400, 24, 128), f32), pltpu.VMEM((400, 24, 128), f32),
            pltpu.VMEM((20 * PITCH, 128), f32), pltpu.VMEM((20 * PITCH, 128), f32), pltpu.VMEM((20 * PITCH, 128), f32),
            pltpu.VMEM((20 * PITCH, 128), f32), pltpu.VMEM((3072, 256), BF),
            pltpu.VMEM((2, 2, 400, 128), BF), pltpu.VMEM((2, 2, 400, 128), BF),
            pltpu.VMEM((2, 2, 400, 128), BF), pltpu.VMEM((2, 2, 400, 128), BF),
            pltpu.VMEM((4, 32, 128), BF), pltpu.VMEM((4, 32, 128), BF),
            pltpu.VMEM((2, 16, 128), f32), pltpu.VMEM((2, 16, 128), f32),
            pltpu.SemaphoreType.DMA((16,)), pltpu.SemaphoreType.DMA((10,)), pltpu.SemaphoreType.DMA((10,))],
        compiler_params=pltpu.CompilerParams(collective_id=2, has_side_effects=True),
        name="transport",
    )(species, diffusivity, cs, velocity.reshape(3, 256, 128), react_index.reshape(1, 4096))


def silu(v):
    half = 0.5 * v
    return (half + half * jnp.tanh(half)).astype(BF)


def network_kernel(count, chem, w1, w2, w3, w4, out):
    out[...] = jnp.zeros_like(out)
    n = count[0, 0]
    slot = lax.broadcasted_iota(jnp.int32, (24, 256), 1)

    def dot(w, v):
        return jnp.dot(w[...], v, preferred_element_type=jnp.float32)

    def body(g, carry):
        where = pl.ds(pl.multiple_of(g * 256, 256), 256)
        h = silu(dot(w1, chem[:, where]))
        h = silu(dot(w2, h))
        h = silu(dot(w3, h))
        r = dot(w4, h)
        out[:, where] = jnp.where(slot + g * 256 < n, r, 0.0).astype(BF)
        return carry
    lax.fori_loop(0, (n + 255) // 256, body, 0)


def network(chem, w1, w2, w3, w4, count):
    vm = pl.BlockSpec(memory_space=pltpu.VMEM)
    return pl.pallas_call(
        network_kernel,
        out_shape=jax.ShapeDtypeStruct((24, 4096), BF),
        in_specs=[pl.BlockSpec(memory_space=pltpu.SMEM)] + [vm] * 5, out_specs=vm,
        name="network",
    )(count, chem, w1, w2, w3, w4)


def real_basis(n):
    k = np.arange(n)
    j = np.arange(n)
    wave = np.where(k <= n // 2, k, k - n // 2)
    ang = 2.0 * np.pi * ((wave[:, None] * j[None, :]) % n) / n
    rows = np.where((k <= n // 2)[:, None], np.cos(ang), np.sin(ang)) * np.sqrt(2.0 / n)
    rows[0] *= np.sqrt(0.5)
    rows[n // 2] *= np.sqrt(0.5)
    lam = 2.0 * np.cos(2.0 * np.pi * wave / n) - 2.0
    return rows.astype(np.float32), lam.astype(np.float32)


def mm(a, b, dims, precision=HI):
    return lax.dot_general(a, b, (dims, ((), ())), precision=precision, preferred_element_type=jnp.float32)


def units(grid, lane):
    turned = []
    for d in range(8):
        w = grid[d]
        for u in range(1, 8):
            w = jnp.where(lane == u, grid[(u + d) % 8], w)
        turned.append(w if d == 0 else pltpu.roll(w, d * 16, 1))
    out = []
    for v in range(8):
        acc = turned[(0 - v) % 8]
        for u in range(1, 8):
            acc = jnp.where(lane == u, turned[(u - v) % 8], acc)
        out.append(acc)
    return out


def finish_kernel(gx_n, gy_n, fields, rates, idx, hr, div, vel, fz, fx, fxt, fy, lamx, lamy, lamz, sout, out,
                  stage, ohot, bhot, sbuf, rbuf, tbuf, pbuf, send_sem, recv_sem, send_sem2, recv_sem2, out_sem):
    gx = lax.axis_index("gx")
    gy = lax.axis_index("gy")
    n = gx_n * gy_n
    me = gx * gy_n + gy
    barrier = pltpu.get_barrier_semaphore()

    def greet(i, c):
        t = lax.rem(me + i, n)
        pl.semaphore_signal(barrier, inc=1, device_id=(t // gy_n, lax.rem(t, gy_n)), device_id_type=MESH)
        return c
    lax.fori_loop(1, n, greet, 0)
    c = idx[...]
    heat_row = jnp.sum(rates[...].astype(jnp.float32) * hr[:, 0:1], axis=0, keepdims=True)
    upper = heat_row.astype(BF).astype(jnp.float32)
    rest = heat_row - upper
    zrow = c % 128
    xyrow = c // 128
    for h in range(2):
        part = upper if h == 0 else rest
        ohot[h * 128:(h + 1) * 128, :] = jnp.where(lax.broadcasted_iota(jnp.int32, (128, 4096), 0) == zrow, part, 0.0).astype(BF)
    bhot[...] = jnp.where(lax.broadcasted_iota(jnp.int32, (256, 4096), 0) == xyrow, 1.0, 0.0).astype(BF)
    both = mm(bhot[...], ohot[...], ((1,), (1,)), None)
    src = div[...] - (both[:, :128] + both[:, 128:])
    zt = mm(fz[...], src, ((1,), (1,)))
    sbuf[:, 0, :] = zt[:, :128]
    sbuf[:, 1, :] = zt[:, 128:]
    pl.semaphore_wait(barrier, n - 1)

    def send(i, c):
        t = lax.rem(me + i, n)
        ta, tb = t // gy_n, lax.rem(t, gy_n)
        pltpu.make_async_remote_copy(
            src_ref=sbuf.at[t], dst_ref=rbuf.at[gy, gx], send_sem=send_sem, recv_sem=recv_sem,
            device_id=(ta, tb), device_id_type=MESH).start()
        return c
    lax.fori_loop(1, n, send, 0)
    own = pltpu.make_async_copy(sbuf.at[me], rbuf.at[gy, gx], recv_sem)
    own.start()
    lane = lax.broadcasted_iota(jnp.int32, (8, 128), 1) // 16
    col = lax.broadcasted_iota(jnp.int32, (8, 128), 1)
    mode = lax.broadcasted_iota(jnp.int32, (1, 128), 1)
    lz = jnp.sum(jnp.where(mode == me, lamz[...], 0.0), axis=1, keepdims=True)
    sym = lamx[...] + lamy[...] + lz
    anchor = (lax.broadcasted_iota(jnp.int32, (128, 256), 0) == 0) & (lax.broadcasted_iota(jnp.int32, (128, 256), 1) == 0) & (me == 0)
    g = jnp.where(anchor, 0.0, 1.0 / jnp.where(anchor, 1.0, sym))
    high = c >= 16384
    xh = jnp.where(high, 15 - c // 2048, c // 2048)
    xyh = xh * 16 + xyrow % 16
    kk = jnp.where(high, 128, 0) + zrow
    bhot[...] = jnp.where(lax.broadcasted_iota(jnp.int32, (256, 4096), 0) == kk, 1.0, 0.0).astype(BF)
    half = (rates[...].astype(jnp.float32) * 0.5).astype(BF)
    flat = stage.reshape(16 * 24 * 16, 128)

    def react(pair):
        rows = [jnp.where(xyh == pair * 16 + q, half, jnp.zeros_like(half)) for q in range(16)]
        rows = jnp.concatenate(rows, axis=0)
        new = fields[pair * 384:(pair + 1) * 384, :] + mm(rows, bhot[...], ((1,), (1,)), None)
        for q in range(16):
            flat[pl.ds(pair * 384 + q, 24, stride=16), :] = new[q * 24:(q + 1) * 24, :128]
            flat[pl.ds((15 - pair) * 384 + q, 24, stride=16), :] = new[q * 24:(q + 1) * 24, 128:]
        for x in (pair, 15 - pair):
            pltpu.make_async_copy(stage.at[x], sout.at[:, x], out_sem.at[x]).start()

    for pair in range(4):
        react(pair)
    pltpu.make_async_copy(rbuf, rbuf, recv_sem).wait()
    pltpu.make_async_copy(sbuf.at[pl.ds(0, n - 1)], sbuf.at[pl.ds(0, n - 1)], send_sem).wait()

    planes = [[None, None] for _ in range(16)]
    for h in range(2):
        for bh in range(2):
            got = units([rbuf[bh * 8 + b, :, h, :] for b in range(8)], lane)
            for xlo in range(8):
                planes[h * 8 + xlo][bh] = got[xlo]
    plane = jnp.concatenate([jnp.concatenate(p, axis=1) for p in planes], axis=0)
    t = mm(fx[...], plane, ((1,), (0,)))
    t = mm(t, fy[...], ((1,), (1,))) * g
    t = mm(t, fy[...], ((1,), (0,)))
    p = mm(fxt[...], t, ((1,), (0,)))
    px = [[p[x * 8:(x + 1) * 8, bh * 128:(bh + 1) * 128] for bh in range(2)] for x in range(16)]
    before = pltpu.roll(p, 1, 1)
    for bh in range(2):
        edge_x = pltpu.roll(px[15][bh], 1, 0)
        edge_y = before[0:8, bh * 128:(bh + 1) * 128]
        for x in range(1, 16):
            edge_y = jnp.where(col % 16 == x, pltpu.roll(before[x * 8:(x + 1) * 8, bh * 128:(bh + 1) * 128], x, 1), edge_y)
        for h in range(2):
            got = units([px[h * 8 + xlo][bh] for xlo in range(8)], lane)
            for b in range(8):
                tbuf[bh * 8 + b, :, h, :] = got[b]
        for b in range(8):
            ex = edge_x if b == 0 else pltpu.roll(edge_x, 128 - b * 16, 1)
            ey = pltpu.roll(edge_y, (128 - b * 16 + 16) % 128, 1) if b != 1 else edge_y
            tbuf[bh * 8 + b, :, 2, :] = jnp.where(lane == 0, ex, ey)

    def back(i, c):
        t = lax.rem(me + i, n)
        ta, tb = t // gy_n, lax.rem(t, gy_n)
        pltpu.make_async_remote_copy(
            src_ref=tbuf.at[tb, ta], dst_ref=pbuf.at[me], send_sem=send_sem2, recv_sem=recv_sem2,
            device_id=(ta, tb), device_id_type=MESH).start()
        return c
    lax.fori_loop(1, n, back, 0)
    own = pltpu.make_async_copy(tbuf.at[gy, gx], pbuf.at[me], recv_sem2)
    own.start()
    for pair in range(4, 8):
        react(pair)
    pltpu.make_async_copy(pbuf, pbuf, recv_sem2).wait()
    pltpu.make_async_copy(pbuf.at[pl.ds(0, n - 1)], pbuf.at[pl.ds(0, n - 1)], send_sem2).wait()
    rows = [mm(pbuf[:, h, :], fz[...], ((0,), (0,))) for h in range(3)]
    q = jnp.concatenate(rows[:2], axis=0)
    west = rows[2][0:16]
    south = rows[2][16:32]
    out[2] = vel[2] - (q - pltpu.roll(q, 1, 1))
    out[0] = vel[0] - (q - jnp.concatenate([west, q[:240]], axis=0))
    sub = lax.broadcasted_iota(jnp.int32, (16, 128), 0)
    for x in range(16):
        cur = q[x * 16:(x + 1) * 16]
        prev = jnp.where(sub == 0, jnp.broadcast_to(south[x:x + 1], (16, 128)), pltpu.roll(cur, 1, 0))
        out[1, x * 16:(x + 1) * 16] = vel[1, x * 16:(x + 1) * 16] - (cur - prev)

    for x in range(16):
        pltpu.make_async_copy(stage.at[x], sout.at[:, x], out_sem.at[x]).wait()


def finish(fields, rates, div, velocity, heat_release, react_index):
    gx_n, gy_n = lax.axis_size("gx"), lax.axis_size("gy")
    fz, lz = real_basis(128)
    fx, lx = real_basis(128)
    fy, ly = real_basis(256)
    fxp = fx.reshape(128, 8, 16).transpose(0, 2, 1).reshape(128, 128)
    vm = pl.BlockSpec(memory_space=pltpu.VMEM)
    hr = jnp.broadcast_to(heat_release[:, None], (24, 128))
    args = (fields, rates, react_index.reshape(1, 4096), hr, div, velocity.reshape(3, 256, 128), jnp.asarray(fz), jnp.asarray(fxp), jnp.asarray(np.ascontiguousarray(fxp.T)), jnp.asarray(fy),
            jnp.asarray(lx[:, None]), jnp.asarray(ly[None, :]), jnp.asarray(lz[None, :]))
    species_out, out = pl.pallas_call(
        functools.partial(finish_kernel, gx_n, gy_n),
        out_shape=(jax.ShapeDtypeStruct((24, 16, 16, 128), jnp.float32), jax.ShapeDtypeStruct((3, 256, 128), jnp.float32)),
        in_specs=[vm] * len(args), out_specs=(pl.BlockSpec(memory_space=pl.ANY), vm),
        scratch_shapes=[
            pltpu.VMEM((16, 24, 16, 128), jnp.float32), pltpu.VMEM((256, 4096), BF), pltpu.VMEM((256, 4096), BF),
            pltpu.VMEM((128, 2, 128), jnp.float32), pltpu.VMEM((16, 8, 2, 128), jnp.float32),
            pltpu.VMEM((16, 8, 3, 128), jnp.float32), pltpu.VMEM((128, 3, 128), jnp.float32),
            pltpu.SemaphoreType.DMA, pltpu.SemaphoreType.DMA, pltpu.SemaphoreType.DMA, pltpu.SemaphoreType.DMA,
            pltpu.SemaphoreType.DMA((16,))],
        compiler_params=pltpu.CompilerParams(collective_id=1, has_side_effects=True),
        name="finish",
    )(*args)
    return species_out, out.reshape(velocity.shape)


def per_device(species, diffusivity, lewis_number, velocity, layer_one, layer_two, layer_three, layer_four,
               heat_release, react_index, react_count):
    fields, chem, div = transport(species, diffusivity, lewis_number, velocity, react_index)
    rates = network(chem, layer_one, layer_two, layer_three, layer_four, react_count)
    return finish(fields, rates, div, velocity, heat_release, react_index)


def solution(mesh):
    return jax.shard_map(
        per_device,
        mesh=mesh,
        in_specs=(
            P(None, "gx", "gy", None),
            P("gx", "gy", None),
            P(),
            P(None, "gx", "gy", None),
            P(),
            P(),
            P(),
            P(),
            P(),
            P("gx", "gy", None),
            P("gx", "gy"),
        ),
        out_specs=(P(None, "gx", "gy", None), P(None, "gx", "gy", None)),
        check_vma=False,
    )
```

```python
import functools

import jax
import jax.numpy as jnp
import numpy as np
from jax import lax
from jax.experimental import pallas as pl
from jax.experimental.pallas import tpu as pltpu
from jax.sharding import PartitionSpec as P

MESH = pl.DeviceIdType.MESH
HI = lax.Precision.HIGHEST
BF = jnp.bfloat16
PITCH = 24


def next_along(v):
    return pltpu.roll(v, 127, 1)


def column(ref):
    rows = lax.broadcasted_iota(jnp.int32, (24, 128), 0)
    out = jnp.zeros((24, 128), jnp.float32)
    for s in range(24):
        out = jnp.where(rows == s, ref[s], out)
    return out


def transport_kernel(gx_n, gy_n, lewis, sp, dif, vel, idx, cnt, fout, gb, div, other,
                     stage, y0, y1, dp, ax, ay, az, sendx, recvx, sendy, recvy, sendc, recvc, sendv, recvv, note,
                     load_sem, ssem, rsem):
    gx = lax.axis_index("gx")
    gy = lax.axis_index("gy")
    east, west = lax.rem(gx + 1, gx_n), lax.rem(gx + gx_n - 1, gx_n)
    north, south = lax.rem(gy + 1, gy_n), lax.rem(gy + gy_n - 1, gy_n)
    mate = gy + 1 - 2 * lax.rem(gy, 2)
    diag = ((east, north), (east, south), (west, north), (west, south))
    barrier = pltpu.get_barrier_semaphore()
    for dev in ((east, gy), (west, gy), (gx, north), (gx, south)) + diag:
        pl.semaphore_signal(barrier, inc=1, device_id=dev, device_id_type=MESH)

    def load(x):
        return pltpu.make_async_copy(sp.at[:, x], stage.at[x], load_sem.at[x])

    def start_load(k, carry):
        load(lax.rem(k + 14, 16)).start()
        return carry
    lax.fori_loop(0, 16, start_load, 0)

    flat = stage.reshape(16 * 24 * 16, 128)

    def copy(src, dst, k, dev):
        return pltpu.make_async_remote_copy(src_ref=src, dst_ref=dst, send_sem=ssem.at[k], recv_sem=rsem.at[k],
                                            device_id=dev, device_id_type=MESH)

    copies = [copy(sendx.at[0], recvx.at[0], 0, (east, gy)), copy(sendx.at[1], recvx.at[1], 1, (west, gy)),
              copy(sendy.at[0], recvy.at[0], 2, (gx, north)), copy(sendy.at[1], recvy.at[1], 3, (gx, south)),
              copy(sendc.at[0], recvc.at[0], 4, diag[0]), copy(sendc.at[1], recvc.at[1], 5, diag[1]),
              copy(sendc.at[2], recvc.at[2], 6, diag[2]), copy(sendc.at[3], recvc.at[3], 7, diag[3]),
              copy(sendv.at[0], recvv.at[0], 8, (west, gy)), copy(sendv.at[1], recvv.at[1], 9, (gx, south)),
              copy(gb.at[0, pl.ds(768, 2304)], gb.at[1, pl.ds(768, 2304)], 10, (gx, mate)),
              copy(gb.at[0, pl.ds(0, 768)], gb.at[1, pl.ds(0, 768)], 11, (gx, mate)),
              copy(note.at[0], other.at[1], 12, (gx, mate))]

    def spread(x):
        load(x).wait()
        for y in range(16):
            y0[(x + 2) * 20 + y + 2] = flat[pl.ds(x * 384 + y, 24, stride=16), :]

    def pack_x(k, carry):
        x = lax.rem(k + 14, 16)
        spread(x)
        for y in range(0, 16, 2):
            two = jnp.concatenate([y0[(x + 2) * 20 + y + 2], y0[(x + 2) * 20 + y + 3]], axis=0)
            sendx[k // 2, lax.rem(k, 2), y * 24:y * 24 + 48, :] = two.astype(BF)
        sendx[k // 2, lax.rem(k, 2), 384:400, :] = dif[pl.ds(pl.multiple_of(x * 16, 16), 16), :].astype(BF)
        return carry
    lax.fori_loop(0, 4, pack_x, 0)
    pl.semaphore_wait(barrier, 8)
    copies[0].start()
    copies[1].start()
    sendv[0] = vel[0, 0:16, :]
    sendv[1] = vel[1, pl.ds(0, 16, stride=16), :]
    copies[8].start()
    copies[9].start()

    def spread_rest(x, carry):
        spread(x)
        return carry
    lax.fori_loop(2, 14, spread_rest, 0)

    def pack_y(k, carry):
        y = lax.rem(k + 14, 16)
        for x in range(0, 16, 2):
            two = jnp.concatenate([y0[(x + 2) * 20 + y + 2], y0[(x + 3) * 20 + y + 2]], axis=0)
            sendy[k // 2, lax.rem(k, 2), x * 24:x * 24 + 48, :] = two.astype(BF)
        sendy[k // 2, lax.rem(k, 2), 384:400, :] = dif[pl.ds(y, 16, stride=16), :].astype(BF)
        return carry
    lax.fori_loop(0, 4, pack_y, 0)
    copies[2].start()
    copies[3].start()
    for k, (x, y) in enumerate(((15, 15), (15, 0), (0, 15), (0, 0))):
        drow = jnp.broadcast_to(dif[x * 16 + y:x * 16 + y + 1, :], (8, 128))
        sendc[k] = jnp.concatenate([y0[(x + 2) * 20 + y + 2], drow], axis=0).astype(BF)
        copies[4 + k].start()
    note[0, 0:1, :] = idx[...].astype(jnp.float32)
    note[0, 1:2, :] = jnp.broadcast_to(cnt[...].astype(jnp.float32), (1, 4096))
    other[0] = note[0]
    copies[12].start()

    for x in range(16):
        dp[pl.ds((x + 2) * PITCH + 2, 16), :] = dif[x * 16:x * 16 + 16, :]

    def conduct():
        d = dp[...]
        ax[...] = 0.5 * (d + jnp.concatenate([d[PITCH:], d[:PITCH]], axis=0))
        ay[...] = 0.5 * (d + pltpu.roll(d, 20 * PITCH - 1, 0))
        az[...] = 0.5 * (d + next_along(d))
    conduct()
    scale = 0.03 / column(lewis)

    def row(ref, r):
        return ref[pl.ds(r, 24, stride=0), :]

    def line(src, i, js):
        c = src[i * 20 + js[0]]
        back = row(ay, i * PITCH + js[0] - 1) * (c - src[i * 20 + js[0] - 1])
        for j in js:
            r = i * PITCH + j
            after = src[i * 20 + j + 1]
            ahead = row(ay, r) * (after - c)
            fx = row(ax, r) * (src[i * 20 + j + 20] - c) - row(ax, r - PITCH) * (c - src[i * 20 + j - 20])
            t = row(az, r) * (next_along(c) - c)
            yield c + scale * (fx + (ahead - back) + (t - pltpu.roll(t, 1, 1)))
            c, back = after, ahead

    def first(n, start, stride, *runs):
        def body(k, carry):
            i = start + stride * k
            for js in runs:
                for j, v in zip(js, line(y0, i, js)):
                    y1[i * 20 + j] = v
            return carry
        lax.fori_loop(0, n, body, 0)

    def second(lo, hi):
        def body(pair, carry):
            js = range(2, 18)
            kept = None
            for j, low, high in zip(js, line(y1, pair + 2, js), line(y1, 17 - pair, js)):
                val = jnp.concatenate([low, high], axis=1)
                base = pl.multiple_of(pair * 384 + (j - 2) * 24, 8)
                fout[pl.ds(base, 24), :] = val
                if j % 2 == 0:
                    kept = val
                else:
                    gb[0, pl.ds(pl.multiple_of(pair * 384 + (j - 3) * 24, 16), 48), :] = jnp.concatenate([kept, val], axis=0).astype(BF)
            return carry
        lax.fori_loop(lo, hi, body, 0)

    first(14, 3, 1, range(3, 17))
    for k in (2, 3):
        copies[k].wait_recv()

    def unpack_y(k, carry):
        d, p = k // 2, lax.rem(k, 2)
        j = p + 18 * d
        for x in range(0, 16, 2):
            two = recvy[d, p, x * 24:x * 24 + 48, :].astype(jnp.float32)
            y0[(x + 2) * 20 + j] = two[:24]
            y0[(x + 3) * 20 + j] = two[24:]
        drows = recvy[d, p, 384:400, :].astype(jnp.float32)
        for x in range(16):
            dp[pl.ds((x + 2) * PITCH + j, 1), :] = drows[x:x + 1]
        return carry
    lax.fori_loop(0, 4, unpack_y, 0)
    conduct()
    first(14, 3, 1, range(1, 3), range(17, 19))
    second(2, 8)
    copies[10].start()
    for k in (0, 1, 4, 5, 6, 7, 8, 9):
        copies[k].wait_recv()

    def unpack_x(k, carry):
        d, p = k // 2, lax.rem(k, 2)
        i = p + 18 * d
        for y in range(0, 16, 2):
            two = recvx[d, p, y * 24:y * 24 + 48, :].astype(jnp.float32)
            y0[i * 20 + y + 2] = two[:24]
            y0[i * 20 + y + 3] = two[24:]
        dp[pl.ds(i * PITCH + 2, 16), :] = recvx[d, p, 384:400, :].astype(jnp.float32)
        return carry
    lax.fori_loop(0, 4, unpack_x, 0)
    for k, (i, j) in enumerate(((1, 1), (1, 18), (18, 1), (18, 18))):
        val = recvc[k].astype(jnp.float32)
        y0[i * 20 + j] = val[:24]
        dp[pl.ds(i * PITCH + j, 1), :] = val[24:25]
    conduct()
    first(2, 1, 17, range(2, 18))
    first(2, 2, 15, range(1, 19))
    second(0, 2)
    copies[11].start()

    sub = lax.broadcasted_iota(jnp.int32, (16, 128), 0)
    for x in range(16):
        here = slice(x * 16, x * 16 + 16)
        nx = recvv[0] if x == 15 else vel[0, x * 16 + 16:x * 16 + 32, :]
        uy = vel[1, here, :]
        ny = jnp.where(sub == 15, jnp.broadcast_to(recvv[1, x:x + 1, :], (16, 128)), pltpu.roll(uy, 15, 0))
        uz = vel[2, here, :]
        div[here, :] = (nx - vel[0, here, :]) + (ny - uy) + (next_along(uz) - uz)
    for k in (10, 11, 12):
        copies[k].wait_recv()
    for c in copies:
        c.wait_send()


def transport(species, diffusivity, lewis_number, velocity, react_index, react_count):
    gx_n, gy_n = lax.axis_size("gx"), lax.axis_size("gy")
    vm = pl.BlockSpec(memory_space=pltpu.VMEM)
    hb = pl.BlockSpec(memory_space=pl.ANY)
    sm = pl.BlockSpec(memory_space=pltpu.SMEM)
    f32 = jnp.float32
    return pl.pallas_call(
        functools.partial(transport_kernel, gx_n, gy_n),
        out_shape=(jax.ShapeDtypeStruct((3072, 256), f32), jax.ShapeDtypeStruct((2, 3072, 256), BF),
                   jax.ShapeDtypeStruct((256, 128), f32), jax.ShapeDtypeStruct((2, 2, 4096), f32)),
        in_specs=[sm, hb, vm, vm, vm, vm], out_specs=(vm, vm, vm, vm),
        scratch_shapes=[
            pltpu.VMEM((16, 24, 16, 128), f32), pltpu.VMEM((400, 24, 128), f32), pltpu.VMEM((400, 24, 128), f32),
            pltpu.VMEM((20 * PITCH, 128), f32), pltpu.VMEM((20 * PITCH, 128), f32), pltpu.VMEM((20 * PITCH, 128), f32),
            pltpu.VMEM((20 * PITCH, 128), f32),
            pltpu.VMEM((2, 2, 400, 128), BF), pltpu.VMEM((2, 2, 400, 128), BF),
            pltpu.VMEM((2, 2, 400, 128), BF), pltpu.VMEM((2, 2, 400, 128), BF),
            pltpu.VMEM((4, 32, 128), BF), pltpu.VMEM((4, 32, 128), BF),
            pltpu.VMEM((2, 16, 128), f32), pltpu.VMEM((2, 16, 128), f32), pltpu.VMEM((1, 2, 4096), f32),
            pltpu.SemaphoreType.DMA((16,)), pltpu.SemaphoreType.DMA((13,)), pltpu.SemaphoreType.DMA((13,))],
        compiler_params=pltpu.CompilerParams(collective_id=2, has_side_effects=True),
        name="transport",
    )(lewis_number, species, diffusivity.reshape(256, 128), velocity.reshape(3, 256, 128), react_index.reshape(1, 4096), react_count)


def silu(v):
    half = 0.5 * v
    return (half + half * jnp.tanh(half)).astype(BF)


def network_kernel(count, notes, gb, w1t, w2, w3, w4, out, w1):
    out[...] = jnp.zeros_like(out)
    w1[...] = jnp.transpose(w1t[...].astype(jnp.float32)).astype(BF)
    mine = count[0, 0]
    theirs = jnp.max(notes[1, 1:2, 0:128]).astype(jnp.int32)
    own = ((mine + 255) // 256 + 1) // 2
    units = own + (theirs + 255) // 256 // 2
    slot = lax.broadcasted_iota(jnp.int32, (24, 256), 1)
    rows256 = lax.broadcasted_iota(jnp.int32, (256, 256), 0)

    def dot(w, v):
        return jnp.dot(w[...], v, preferred_element_type=jnp.float32)

    def gather(which, where):
        c = notes[which, 0:1, where].astype(jnp.int32)
        x = c // 2048
        high = x >= 8
        xyh = jnp.where(high, 15 - x, x) * 16 + (c // 128) % 16
        kk = jnp.where(high, 128, 0) + c % 128
        pick = jnp.where(rows256 == kk, 1.0, 0.0).astype(BF)
        acc = jnp.zeros((24, 256), jnp.float32)
        for part in range(2):
            t = dot(gb.at[which, part * 1536:(part + 1) * 1536, :], pick)
            for q in range(64):
                acc = acc + jnp.where(xyh == part * 64 + q, t[q * 24:(q + 1) * 24], 0.0)
        return acc.astype(BF)

    def body(it, carry):
        places = []
        for k in range(2):
            t = jnp.minimum(2 * it + k, units - 1)
            which = (t >= own).astype(jnp.int32)
            unit = jnp.where(t >= own, 2 * (t - own) + 1, 2 * t)
            places.append((which, unit, pl.ds(pl.multiple_of(unit * 256, 256), 256)))
        hs = [gather(which, where) for which, _, where in places]
        hs = [silu(dot(w1, h)) for h in hs]
        hs = [silu(dot(w2, h)) for h in hs]
        hs = [silu(dot(w3, h)) for h in hs]
        for (which, unit, where), h in zip(places, hs):
            limit = jnp.where(which == 0, mine, theirs)
            out[which, :, where] = jnp.where(slot + unit * 256 < limit, dot(w4, h), 0.0).astype(BF)
        return carry
    lax.fori_loop(0, (units + 1) // 2, body, 0)


def network(notes, gb, w1, w2, w3, w4, count):
    vm = pl.BlockSpec(memory_space=pltpu.VMEM)
    return pl.pallas_call(
        network_kernel,
        out_shape=jax.ShapeDtypeStruct((2, 24, 4096), BF),
        in_specs=[pl.BlockSpec(memory_space=pltpu.SMEM)] + [vm] * 6, out_specs=vm,
        scratch_shapes=[pltpu.VMEM((1600, 24), BF)],
        name="network",
    )(count, notes, gb, w1.T, w2, w3, w4)


def real_basis(n):
    k = np.arange(n)
    j = np.arange(n)
    wave = np.where(k <= n // 2, k, k - n // 2)
    ang = 2.0 * np.pi * ((wave[:, None] * j[None, :]) % n) / n
    rows = np.where((k <= n // 2)[:, None], np.cos(ang), np.sin(ang)) * np.sqrt(2.0 / n)
    rows[0] *= np.sqrt(0.5)
    rows[n // 2] *= np.sqrt(0.5)
    lam = 2.0 * np.cos(2.0 * np.pi * wave / n) - 2.0
    return rows.astype(np.float32), lam.astype(np.float32)


def mm(a, b, dims, precision=HI):
    return lax.dot_general(a, b, (dims, ((), ())), precision=precision, preferred_element_type=jnp.float32)


def units(grid, lane):
    turned = []
    for d in range(8):
        w = grid[d]
        for u in range(1, 8):
            w = jnp.where(lane == u, grid[(u + d) % 8], w)
        turned.append(w if d == 0 else pltpu.roll(w, d * 16, 1))
    out = []
    for v in range(8):
        acc = turned[(0 - v) % 8]
        for u in range(1, 8):
            acc = jnp.where(lane == u, turned[(u - v) % 8], acc)
        out.append(acc)
    return out


def finish_kernel(gx_n, gy_n, heat_release, fields, shares, idx, div, vel, fz, fx, fxt, fy, lamx, lamy, lamz, sout, out,
                  stage, ohot, bhot, theirs, sbuf, rbuf, tbuf, pbuf, send_sem, recv_sem, send_sem2, recv_sem2, out_sem, swap_sem):
    gx = lax.axis_index("gx")
    gy = lax.axis_index("gy")
    n = gx_n * gy_n
    me = gx * gy_n + gy
    barrier = pltpu.get_barrier_semaphore()

    def greet(i, c):
        t = lax.rem(me + i, n)
        pl.semaphore_signal(barrier, inc=1, device_id=(t // gy_n, lax.rem(t, gy_n)), device_id_type=MESH)
        return c
    lax.fori_loop(1, n, greet, 0)
    c = idx[...]
    zrow = c % 128
    xyrow = c // 128
    bhot[...] = jnp.where(lax.broadcasted_iota(jnp.int32, (256, 4096), 0) == xyrow, 1.0, 0.0).astype(BF)
    pl.semaphore_wait(barrier, n - 1)
    swap = pltpu.make_async_remote_copy(
        src_ref=shares.at[1], dst_ref=theirs, send_sem=swap_sem.at[0], recv_sem=swap_sem.at[1],
        device_id=(gx, gy + 1 - 2 * lax.rem(gy, 2)), device_id_type=MESH)
    swap.start()
    heat_column = column(heat_release)[:, 0:1]
    swap.wait()
    rates = shares[0].astype(jnp.float32) + theirs[...].astype(jnp.float32)
    heat_row = jnp.sum(rates * heat_column, axis=0, keepdims=True)
    upper = heat_row.astype(BF).astype(jnp.float32)
    rest = heat_row - upper
    for h in range(2):
        part = upper if h == 0 else rest
        ohot[h * 128:(h + 1) * 128, :] = jnp.where(lax.broadcasted_iota(jnp.int32, (128, 4096), 0) == zrow, part, 0.0).astype(BF)
    both = mm(bhot[...], ohot[...], ((1,), (1,)), None)
    src = div[...] - (both[:, :128] + both[:, 128:])
    zt = mm(fz[...], src, ((1,), (1,)))
    sbuf[:, 0, :] = zt[:, :128]
    sbuf[:, 1, :] = zt[:, 128:]

    def send(i, c):
        t = lax.rem(me + i, n)
        ta, tb = t // gy_n, lax.rem(t, gy_n)
        pltpu.make_async_remote_copy(
            src_ref=sbuf.at[t], dst_ref=rbuf.at[gy, gx], send_sem=send_sem, recv_sem=recv_sem,
            device_id=(ta, tb), device_id_type=MESH).start()
        return c
    lax.fori_loop(1, n, send, 0)
    own = pltpu.make_async_copy(sbuf.at[me], rbuf.at[gy, gx], recv_sem)
    own.start()
    lane = lax.broadcasted_iota(jnp.int32, (8, 128), 1) // 16
    col = lax.broadcasted_iota(jnp.int32, (8, 128), 1)
    mode = lax.broadcasted_iota(jnp.int32, (1, 128), 1)
    lz = jnp.sum(jnp.where(mode == me, lamz[...], 0.0), axis=1, keepdims=True)
    sym = lamx[...] + lamy[...] + lz
    anchor = (lax.broadcasted_iota(jnp.int32, (128, 256), 0) == 0) & (lax.broadcasted_iota(jnp.int32, (128, 256), 1) == 0) & (me == 0)
    g = jnp.where(anchor, 0.0, 1.0 / jnp.where(anchor, 1.0, sym))
    high = c >= 16384
    xh = jnp.where(high, 15 - c // 2048, c // 2048)
    xyh = xh * 16 + xyrow % 16
    kk = jnp.where(high, 128, 0) + zrow
    bhot[...] = jnp.where(lax.broadcasted_iota(jnp.int32, (256, 4096), 0) == kk, 1.0, 0.0).astype(BF)
    half = (rates * 0.5).astype(BF)
    flat = stage.reshape(16 * 24 * 16, 128)

    def react(pair):
        rows = [jnp.where(xyh == pair * 16 + q, half, jnp.zeros_like(half)) for q in range(16)]
        rows = jnp.concatenate(rows, axis=0)
        new = fields[pair * 384:(pair + 1) * 384, :] + mm(rows, bhot[...], ((1,), (1,)), None)
        for q in range(16):
            flat[pl.ds(pair * 384 + q, 24, stride=16), :] = new[q * 24:(q + 1) * 24, :128]
            flat[pl.ds((15 - pair) * 384 + q, 24, stride=16), :] = new[q * 24:(q + 1) * 24, 128:]
        for x in (pair, 15 - pair):
            pltpu.make_async_copy(stage.at[x], sout.at[:, x], out_sem.at[x]).start()

    for pair in range(4):
        react(pair)
    pltpu.make_async_copy(rbuf, rbuf, recv_sem).wait()
    pltpu.make_async_copy(sbuf.at[pl.ds(0, n - 1)], sbuf.at[pl.ds(0, n - 1)], send_sem).wait()

    planes = [[None, None] for _ in range(16)]
    for h in range(2):
        for bh in range(2):
            got = units([rbuf[bh * 8 + b, :, h, :] for b in range(8)], lane)
            for xlo in range(8):
                planes[h * 8 + xlo][bh] = got[xlo]
    plane = jnp.concatenate([jnp.concatenate(p, axis=1) for p in planes], axis=0)
    t = mm(fx[...], plane, ((1,), (0,)))
    t = mm(t, fy[...], ((1,), (1,))) * g
    t = mm(t, fy[...], ((1,), (0,)))
    p = mm(fxt[...], t, ((1,), (0,)))
    px = [[p[x * 8:(x + 1) * 8, bh * 128:(bh + 1) * 128] for bh in range(2)] for x in range(16)]
    before = pltpu.roll(p, 1, 1)
    for bh in range(2):
        edge_x = pltpu.roll(px[15][bh], 1, 0)
        edge_y = before[0:8, bh * 128:(bh + 1) * 128]
        for x in range(1, 16):
            edge_y = jnp.where(col % 16 == x, pltpu.roll(before[x * 8:(x + 1) * 8, bh * 128:(bh + 1) * 128], x, 1), edge_y)
        for h in range(2):
            got = units([px[h * 8 + xlo][bh] for xlo in range(8)], lane)
            for b in range(8):
                tbuf[bh * 8 + b, :, h, :] = got[b]
        for b in range(8):
            ex = edge_x if b == 0 else pltpu.roll(edge_x, 128 - b * 16, 1)
            ey = pltpu.roll(edge_y, (128 - b * 16 + 16) % 128, 1) if b != 1 else edge_y
            tbuf[bh * 8 + b, :, 2, :] = jnp.where(lane == 0, ex, ey)

    def back(i, c):
        t = lax.rem(me + i, n)
        ta, tb = t // gy_n, lax.rem(t, gy_n)
        pltpu.make_async_remote_copy(
            src_ref=tbuf.at[tb, ta], dst_ref=pbuf.at[me], send_sem=send_sem2, recv_sem=recv_sem2,
            device_id=(ta, tb), device_id_type=MESH).start()
        return c
    lax.fori_loop(1, n, back, 0)
    own = pltpu.make_async_copy(tbuf.at[gy, gx], pbuf.at[me], recv_sem2)
    own.start()
    for pair in range(4, 8):
        react(pair)
    pltpu.make_async_copy(pbuf, pbuf, recv_sem2).wait()
    pltpu.make_async_copy(pbuf.at[pl.ds(0, n - 1)], pbuf.at[pl.ds(0, n - 1)], send_sem2).wait()
    rows = [mm(pbuf[:, h, :], fz[...], ((0,), (0,))) for h in range(3)]
    q = jnp.concatenate(rows[:2], axis=0)
    west = rows[2][0:16]
    south = rows[2][16:32]
    out[2] = vel[2] - (q - pltpu.roll(q, 1, 1))
    out[0] = vel[0] - (q - jnp.concatenate([west, q[:240]], axis=0))
    sub = lax.broadcasted_iota(jnp.int32, (16, 128), 0)
    for x in range(16):
        cur = q[x * 16:(x + 1) * 16]
        prev = jnp.where(sub == 0, jnp.broadcast_to(south[x:x + 1], (16, 128)), pltpu.roll(cur, 1, 0))
        out[1, x * 16:(x + 1) * 16] = vel[1, x * 16:(x + 1) * 16] - (cur - prev)

    for x in range(16):
        pltpu.make_async_copy(stage.at[x], sout.at[:, x], out_sem.at[x]).wait()


def finish(fields, shares, div, velocity, heat_release, react_index):
    gx_n, gy_n = lax.axis_size("gx"), lax.axis_size("gy")
    fz, lz = real_basis(128)
    fx, lx = real_basis(128)
    fy, ly = real_basis(256)
    fxp = fx.reshape(128, 8, 16).transpose(0, 2, 1).reshape(128, 128)
    vm = pl.BlockSpec(memory_space=pltpu.VMEM)
    args = (heat_release, fields, shares, react_index.reshape(1, 4096), div, velocity.reshape(3, 256, 128), jnp.asarray(fz), jnp.asarray(fxp), jnp.asarray(np.ascontiguousarray(fxp.T)), jnp.asarray(fy),
            jnp.asarray(lx[:, None]), jnp.asarray(ly[None, :]), jnp.asarray(lz[None, :]))
    species_out, out = pl.pallas_call(
        functools.partial(finish_kernel, gx_n, gy_n),
        out_shape=(jax.ShapeDtypeStruct((24, 16, 16, 128), jnp.float32), jax.ShapeDtypeStruct((3, 256, 128), jnp.float32)),
        in_specs=[pl.BlockSpec(memory_space=pltpu.SMEM)] + [vm] * (len(args) - 1), out_specs=(pl.BlockSpec(memory_space=pl.ANY), vm),
        scratch_shapes=[
            pltpu.VMEM((16, 24, 16, 128), jnp.float32), pltpu.VMEM((256, 4096), BF), pltpu.VMEM((256, 4096), BF), pltpu.VMEM((24, 4096), BF),
            pltpu.VMEM((128, 2, 128), jnp.float32), pltpu.VMEM((16, 8, 2, 128), jnp.float32),
            pltpu.VMEM((16, 8, 3, 128), jnp.float32), pltpu.VMEM((128, 3, 128), jnp.float32),
            pltpu.SemaphoreType.DMA, pltpu.SemaphoreType.DMA, pltpu.SemaphoreType.DMA, pltpu.SemaphoreType.DMA,
            pltpu.SemaphoreType.DMA((16,)), pltpu.SemaphoreType.DMA((2,))],
        compiler_params=pltpu.CompilerParams(collective_id=1, has_side_effects=True),
        name="finish",
    )(*args)
    return species_out, out.reshape(velocity.shape)


def per_device(species, diffusivity, lewis_number, velocity, layer_one, layer_two, layer_three, layer_four,
               heat_release, react_index, react_count):
    fields, gb, div, notes = transport(species, diffusivity, lewis_number, velocity, react_index, react_count)
    shares = network(notes, gb, layer_one, layer_two, layer_three, layer_four, react_count)
    return finish(fields, shares, div, velocity, heat_release, react_index)


def solution(mesh):
    return jax.shard_map(
        per_device,
        mesh=mesh,
        in_specs=(
            P(None, "gx", "gy", None),
            P("gx", "gy", None),
            P(),
            P(None, "gx", "gy", None),
            P(),
            P(),
            P(),
            P(),
            P(),
            P("gx", "gy", None),
            P("gx", "gy"),
        ),
        out_specs=(P(None, "gx", "gy", None), P(None, "gx", "gy", None)),
        check_vma=False,
    )
```

```python
import functools

import jax
import jax.numpy as jnp
import numpy as np
from jax import lax
from jax.experimental import pallas as pl
from jax.experimental.pallas import tpu as pltpu
from jax.sharding import PartitionSpec as P

MESH = pl.DeviceIdType.MESH
HI = lax.Precision.HIGHEST
BF = jnp.bfloat16
PITCH = 24


def next_along(v):
    return pltpu.roll(v, 127, 1)


def column(ref):
    rows = lax.broadcasted_iota(jnp.int32, (24, 128), 0)
    out = jnp.zeros((24, 128), jnp.float32)
    for s in range(24):
        out = jnp.where(rows == s, ref[s], out)
    return out


def transport_kernel(gx_n, gy_n, lewis, sp, dif, vel_in, idx, cnt, shift, fields, field_pair, div, other,
                     stage, y0, y1, dp, ax, ay, az, sendx, recvx, sendy, recvy, sendc, recvc, sendv, recvv, note,
                     fout, gb, vel, azm, load_sem, ssem, rsem, out_sem):
    gx = lax.axis_index("gx")
    gy = lax.axis_index("gy")
    east, west = lax.rem(gx + 1, gx_n), lax.rem(gx + gx_n - 1, gx_n)
    north, south = lax.rem(gy + 1, gy_n), lax.rem(gy + gy_n - 1, gy_n)
    mate = gy + 1 - 2 * lax.rem(gy, 2)
    diag = ((east, north), (east, south), (west, north), (west, south))
    barrier = pltpu.get_barrier_semaphore()
    for dev in ((east, gy), (west, gy), (gx, north), (gx, south)) + diag:
        pl.semaphore_signal(barrier, inc=1, device_id=dev, device_id_type=MESH)

    def load(x):
        return pltpu.make_async_copy(sp.at[:, x], stage.at[x], load_sem.at[x])

    def start_load(k, carry):
        load(lax.rem(k + 14, 16)).start()
        return carry
    lax.fori_loop(0, 16, start_load, 0)
    load_flow = pltpu.make_async_copy(vel_in, vel, out_sem.at[4])
    load_flow.start()

    flat = stage.reshape(16 * 24 * 16, 128)

    def copy(src, dst, k, dev):
        return pltpu.make_async_remote_copy(src_ref=src, dst_ref=dst, send_sem=ssem.at[k], recv_sem=rsem.at[k],
                                            device_id=dev, device_id_type=MESH)

    copies = [copy(sendx.at[0], recvx.at[0], 0, (east, gy)), copy(sendx.at[1], recvx.at[1], 1, (west, gy)),
              copy(sendy.at[0], recvy.at[0], 2, (gx, north)), copy(sendy.at[1], recvy.at[1], 3, (gx, south)),
              copy(sendc.at[0], recvc.at[0], 4, diag[0]), copy(sendc.at[1], recvc.at[1], 5, diag[1]),
              copy(sendc.at[2], recvc.at[2], 6, diag[2]), copy(sendc.at[3], recvc.at[3], 7, diag[3]),
              copy(sendv.at[0], recvv.at[0], 8, (west, gy)), copy(sendv.at[1], recvv.at[1], 9, (gx, south)),
              copy(gb.at[pl.ds(768, 2304)], field_pair.at[1, pl.ds(768, 2304)], 10, (gx, mate)),
              copy(gb.at[pl.ds(0, 768)], field_pair.at[1, pl.ds(0, 768)], 11, (gx, mate)),
              copy(note.at[0], other.at[1], 12, (gx, mate))]

    def spread(x):
        load(x).wait()
        for y in range(16):
            y0[(x + 2) * 20 + y + 2] = flat[pl.ds(x * 384 + y, 24, stride=16), :]

    def pack_x(k, carry):
        x = lax.rem(k + 14, 16)
        spread(x)
        for y in range(0, 16, 2):
            two = jnp.concatenate([y0[(x + 2) * 20 + y + 2], y0[(x + 2) * 20 + y + 3]], axis=0)
            sendx[k // 2, lax.rem(k, 2), y * 24:y * 24 + 48, :] = two.astype(BF)
        sendx[k // 2, lax.rem(k, 2), 384:400, :] = dif[pl.ds(pl.multiple_of(x * 16, 16), 16), :].astype(BF)
        return carry
    lax.fori_loop(0, 4, pack_x, 0)
    pl.semaphore_wait(barrier, 8)
    copies[0].start()
    copies[1].start()
    load_flow.wait()
    sendv[0] = vel[0, 0:16, :]
    sendv[1] = vel[1, pl.ds(0, 16, stride=16), :]
    copies[8].start()
    copies[9].start()

    def spread_rest(x, carry):
        spread(x)
        return carry
    lax.fori_loop(2, 14, spread_rest, 0)

    def pack_y(k, carry):
        y = lax.rem(k + 14, 16)
        for x in range(0, 16, 2):
            two = jnp.concatenate([y0[(x + 2) * 20 + y + 2], y0[(x + 3) * 20 + y + 2]], axis=0)
            sendy[k // 2, lax.rem(k, 2), x * 24:x * 24 + 48, :] = two.astype(BF)
        sendy[k // 2, lax.rem(k, 2), 384:400, :] = dif[pl.ds(y, 16, stride=16), :].astype(BF)
        return carry
    lax.fori_loop(0, 4, pack_y, 0)
    copies[2].start()
    copies[3].start()
    for k, (x, y) in enumerate(((15, 15), (15, 0), (0, 15), (0, 0))):
        drow = jnp.broadcast_to(dif[x * 16 + y:x * 16 + y + 1, :], (8, 128))
        sendc[k] = jnp.concatenate([y0[(x + 2) * 20 + y + 2], drow], axis=0).astype(BF)
        copies[4 + k].start()
    note[0, 0:1, :] = idx[...].astype(jnp.float32)
    note[0, 1:2, :] = jnp.broadcast_to(cnt[...].astype(jnp.float32), (1, 4096))
    other[0] = note[0]
    copies[12].start()

    for x in range(16):
        dp[pl.ds((x + 2) * PITCH + 2, 16), :] = dif[x * 16:x * 16 + 16, :]

    def conduct():
        d = dp[...]
        ax[...] = 0.5 * (d + jnp.concatenate([d[PITCH:], d[:PITCH]], axis=0))
        ay[...] = 0.5 * (d + pltpu.roll(d, 20 * PITCH - 1, 0))
        up = 0.5 * (d + next_along(d))
        az[...] = up
        azm[...] = pltpu.roll(up, 1, 1)
    conduct()
    scale = 0.03 / column(lewis)

    def row(ref, r):
        return ref[pl.ds(r, 24, stride=0), :]

    def line(src, i, js):
        c = src[i * 20 + js[0]]
        if len(js) > 2:
            block = src[pl.ds(i * 20 + js[0], len(js))].reshape(len(js) * 24, 128)
            upper = block.astype(BF)
            rest = (block - upper.astype(jnp.float32)).astype(BF)
            dz = jnp.dot(jnp.concatenate([upper, rest], axis=1), shift[...], preferred_element_type=jnp.float32)
        back = row(ay, i * PITCH + js[0] - 1) * (c - src[i * 20 + js[0] - 1])
        for j in js:
            r = i * PITCH + j
            after = src[i * 20 + j + 1]
            ahead = row(ay, r) * (after - c)
            fx = row(ax, r) * (src[i * 20 + j + 20] - c) - row(ax, r - PITCH) * (c - src[i * 20 + j - 20])
            if len(js) > 2:
                at = (j - js[0]) * 24
                fz = row(az, r) * dz[at:at + 24, :128] - row(azm, r) * dz[at:at + 24, 128:]
            else:
                t = row(az, r) * (next_along(c) - c)
                fz = t - pltpu.roll(t, 1, 1)
            yield c + scale * (fx + (ahead - back) + fz)
            c, back = after, ahead

    def first(n, start, stride, *runs):
        def body(k, carry):
            i = start + stride * k
            for js in runs:
                for j, v in zip(js, line(y0, i, js)):
                    y1[i * 20 + j] = v
            return carry
        lax.fori_loop(0, n, body, 0)

    def second(lo, hi):
        def body(pair, carry):
            js = range(2, 18)
            kept = None
            for j, low, high in zip(js, line(y1, pair + 2, js), line(y1, 17 - pair, js)):
                val = jnp.concatenate([low, high], axis=1)
                base = pl.multiple_of(pair * 384 + (j - 2) * 24, 8)
                fout[pl.ds(base, 24), :] = val
                if j % 2 == 0:
                    kept = val
                else:
                    gb[pl.ds(pl.multiple_of(pair * 384 + (j - 3) * 24, 16), 48), :] = jnp.concatenate([kept, val], axis=0).astype(BF)
            return carry
        lax.fori_loop(lo, hi, body, 0)

    first(14, 3, 1, range(3, 17))
    for k in (2, 3):
        copies[k].wait_recv()

    def unpack_y(k, carry):
        d, p = k // 2, lax.rem(k, 2)
        j = p + 18 * d
        for x in range(0, 16, 2):
            two = recvy[d, p, x * 24:x * 24 + 48, :].astype(jnp.float32)
            y0[(x + 2) * 20 + j] = two[:24]
            y0[(x + 3) * 20 + j] = two[24:]
        drows = recvy[d, p, 384:400, :].astype(jnp.float32)
        for x in range(16):
            dp[pl.ds((x + 2) * PITCH + j, 1), :] = drows[x:x + 1]
        return carry
    lax.fori_loop(0, 4, unpack_y, 0)
    conduct()
    first(14, 3, 1, range(1, 3), range(17, 19))
    second(2, 8)
    copies[10].start()
    stores = [pltpu.make_async_copy(gb.at[pl.ds(768, 2304)], field_pair.at[0, pl.ds(768, 2304)], out_sem.at[0]),
              pltpu.make_async_copy(fout.at[pl.ds(768, 2304)], fields.at[pl.ds(768, 2304)], out_sem.at[1]),
              pltpu.make_async_copy(gb.at[pl.ds(0, 768)], field_pair.at[0, pl.ds(0, 768)], out_sem.at[2]),
              pltpu.make_async_copy(fout.at[pl.ds(0, 768)], fields.at[pl.ds(0, 768)], out_sem.at[3])]
    stores[0].start()
    stores[1].start()
    for k in (0, 1, 4, 5, 6, 7, 8, 9):
        copies[k].wait_recv()

    def unpack_x(k, carry):
        d, p = k // 2, lax.rem(k, 2)
        i = p + 18 * d
        for y in range(0, 16, 2):
            two = recvx[d, p, y * 24:y * 24 + 48, :].astype(jnp.float32)
            y0[i * 20 + y + 2] = two[:24]
            y0[i * 20 + y + 3] = two[24:]
        dp[pl.ds(i * PITCH + 2, 16), :] = recvx[d, p, 384:400, :].astype(jnp.float32)
        return carry
    lax.fori_loop(0, 4, unpack_x, 0)
    for k, (i, j) in enumerate(((1, 1), (1, 18), (18, 1), (18, 18))):
        val = recvc[k].astype(jnp.float32)
        y0[i * 20 + j] = val[:24]
        dp[pl.ds(i * PITCH + j, 1), :] = val[24:25]
    conduct()
    first(2, 1, 17, range(2, 18))
    first(2, 2, 15, range(1, 19))
    second(0, 2)
    copies[11].start()
    stores[2].start()
    stores[3].start()

    sub = lax.broadcasted_iota(jnp.int32, (16, 128), 0)
    for x in range(16):
        here = slice(x * 16, x * 16 + 16)
        nx = recvv[0] if x == 15 else vel[0, x * 16 + 16:x * 16 + 32, :]
        uy = vel[1, here, :]
        ny = jnp.where(sub == 15, jnp.broadcast_to(recvv[1, x:x + 1, :], (16, 128)), pltpu.roll(uy, 15, 0))
        uz = vel[2, here, :]
        div[here, :] = (nx - vel[0, here, :]) + (ny - uy) + (next_along(uz) - uz)
    for k in (10, 11, 12):
        copies[k].wait_recv()
    for c in copies:
        c.wait_send()
    for c in stores:
        c.wait()


def transport(species, diffusivity, lewis_number, velocity, react_index, react_count):
    gx_n, gy_n = lax.axis_size("gx"), lax.axis_size("gy")
    vm = pl.BlockSpec(memory_space=pltpu.VMEM)
    hb = pl.BlockSpec(memory_space=pl.ANY)
    sm = pl.BlockSpec(memory_space=pltpu.SMEM)
    f32 = jnp.float32
    ahead = np.roll(np.eye(128), 1, 0) - np.eye(128)
    behind = np.eye(128) - np.roll(np.eye(128), -1, 0)
    shift = np.tile(np.concatenate([ahead, behind], axis=1), (2, 1))
    return pl.pallas_call(
        functools.partial(transport_kernel, gx_n, gy_n),
        out_shape=(jax.ShapeDtypeStruct((3072, 256), f32), jax.ShapeDtypeStruct((2, 3072, 256), BF),
                   jax.ShapeDtypeStruct((256, 128), f32), jax.ShapeDtypeStruct((2, 2, 4096), f32)),
        in_specs=[sm, hb, vm, hb, vm, vm, vm], out_specs=(hb, hb, vm, vm),
        scratch_shapes=[
            pltpu.VMEM((16, 24, 16, 128), f32), pltpu.VMEM((400, 24, 128), f32), pltpu.VMEM((400, 24, 128), f32),
            pltpu.VMEM((20 * PITCH, 128), f32), pltpu.VMEM((20 * PITCH, 128), f32), pltpu.VMEM((20 * PITCH, 128), f32),
            pltpu.VMEM((20 * PITCH, 128), f32),
            pltpu.VMEM((2, 2, 400, 128), BF), pltpu.VMEM((2, 2, 400, 128), BF),
            pltpu.VMEM((2, 2, 400, 128), BF), pltpu.VMEM((2, 2, 400, 128), BF),
            pltpu.VMEM((4, 32, 128), BF), pltpu.VMEM((4, 32, 128), BF),
            pltpu.VMEM((2, 16, 128), f32), pltpu.VMEM((2, 16, 128), f32), pltpu.VMEM((1, 2, 4096), f32),
            pltpu.VMEM((3072, 256), f32), pltpu.VMEM((3072, 256), BF), pltpu.VMEM((3, 256, 128), f32), pltpu.VMEM((20 * PITCH, 128), f32),
            pltpu.SemaphoreType.DMA((16,)), pltpu.SemaphoreType.DMA((13,)), pltpu.SemaphoreType.DMA((13,)),
            pltpu.SemaphoreType.DMA((5,))],
        compiler_params=pltpu.CompilerParams(collective_id=2, has_side_effects=True),
        name="transport",
    )(lewis_number, species, diffusivity.reshape(256, 128), velocity.reshape(3, 256, 128), react_index.reshape(1, 4096), react_count, jnp.asarray(shift, BF))


def silu(v):
    half = 0.5 * v
    return (half + half * jnp.tanh(half)).astype(BF)


def network_kernel(count, notes, gb, w1t, w2, w3, w4, out, w1):
    out[...] = jnp.zeros_like(out)
    w1[...] = jnp.transpose(w1t[...].astype(jnp.float32)).astype(BF)
    mine = count[0, 0]
    theirs = jnp.max(notes[1, 1:2, 0:128]).astype(jnp.int32)
    own = ((mine + 255) // 256 + 1) // 2
    units = own + (theirs + 255) // 256 // 2
    slot = lax.broadcasted_iota(jnp.int32, (24, 256), 1)
    rows256 = lax.broadcasted_iota(jnp.int32, (256, 256), 0)

    def dot(w, v):
        return jnp.dot(w[...], v, preferred_element_type=jnp.float32)

    def gather(which, where):
        c = notes[which, 0:1, where].astype(jnp.int32)
        x = c // 2048
        high = x >= 8
        xyh = jnp.where(high, 15 - x, x) * 16 + (c // 128) % 16
        kk = jnp.where(high, 128, 0) + c % 128
        pick = jnp.where(rows256 == kk, 1.0, 0.0).astype(BF)
        acc = jnp.zeros((24, 256), jnp.float32)
        for part in range(2):
            t = dot(gb.at[which, part * 1536:(part + 1) * 1536, :], pick)
            for q in range(64):
                acc = acc + jnp.where(xyh == part * 64 + q, t[q * 24:(q + 1) * 24], 0.0)
        return acc.astype(BF)

    def body(it, carry):
        places = []
        for k in range(2):
            t = jnp.minimum(2 * it + k, units - 1)
            which = (t >= own).astype(jnp.int32)
            unit = jnp.where(t >= own, 2 * (t - own) + 1, 2 * t)
            places.append((which, unit, pl.ds(pl.multiple_of(unit * 256, 256), 256)))
        hs = [gather(which, where) for which, _, where in places]
        hs = [silu(dot(w1, h)) for h in hs]
        hs = [silu(dot(w2, h)) for h in hs]
        hs = [silu(dot(w3, h)) for h in hs]
        for (which, unit, where), h in zip(places, hs):
            limit = jnp.where(which == 0, mine, theirs)
            out[which, :, where] = jnp.where(slot + unit * 256 < limit, dot(w4, h), 0.0).astype(BF)
        return carry
    lax.fori_loop(0, (units + 1) // 2, body, 0)


def network(notes, gb, w1, w2, w3, w4, count):
    vm = pl.BlockSpec(memory_space=pltpu.VMEM)
    return pl.pallas_call(
        network_kernel,
        out_shape=jax.ShapeDtypeStruct((2, 24, 4096), BF),
        in_specs=[pl.BlockSpec(memory_space=pltpu.SMEM)] + [vm] * 6, out_specs=vm,
        scratch_shapes=[pltpu.VMEM((1600, 24), BF)],
        name="network",
    )(count, notes, gb, w1.T, w2, w3, w4)


def real_basis(n):
    k = np.arange(n)
    j = np.arange(n)
    wave = np.where(k <= n // 2, k, k - n // 2)
    ang = 2.0 * np.pi * ((wave[:, None] * j[None, :]) % n) / n
    rows = np.where((k <= n // 2)[:, None], np.cos(ang), np.sin(ang)) * np.sqrt(2.0 / n)
    rows[0] *= np.sqrt(0.5)
    rows[n // 2] *= np.sqrt(0.5)
    lam = 2.0 * np.cos(2.0 * np.pi * wave / n) - 2.0
    return rows.astype(np.float32), lam.astype(np.float32)


def mm(a, b, dims, precision=HI):
    return lax.dot_general(a, b, (dims, ((), ())), precision=precision, preferred_element_type=jnp.float32)


def units(grid, lane):
    turned = []
    for d in range(8):
        w = grid[d]
        for u in range(1, 8):
            w = jnp.where(lane == u, grid[(u + d) % 8], w)
        turned.append(w if d == 0 else pltpu.roll(w, d * 16, 1))
    out = []
    for v in range(8):
        acc = turned[(0 - v) % 8]
        for u in range(1, 8):
            acc = jnp.where(lane == u, turned[(u - v) % 8], acc)
        out.append(acc)
    return out


def finish_kernel(gx_n, gy_n, heat_release, fields, shares, idx, div, vel, fz, fx, fxt, fy, lamx, lamy, lamz, sout, out,
                  stage, ohot, bhot, theirs, sbuf, rbuf, tbuf, pbuf, send_sem, recv_sem, send_sem2, recv_sem2, out_sem, swap_sem, load_sem, field, flow, word):
    gx = lax.axis_index("gx")
    gy = lax.axis_index("gy")
    n = gx_n * gy_n
    me = gx * gy_n + gy
    barrier = pltpu.get_barrier_semaphore()

    def everyone(act):
        def rows_of(i, carry):
            ta = lax.rem(gx + i, gx_n)
            for j in range(gy_n):
                act(ta, lax.rem(gy + j, gy_n))
            return carry
        lax.fori_loop(1, gx_n, rows_of, 0)
        for j in range(1, gy_n):
            act(gx, lax.rem(gy + j, gy_n))

    for j in range(1, gx_n):
        pl.semaphore_signal(barrier, inc=1, device_id=(lax.rem(gx + j, gx_n), gy), device_id_type=MESH)
    for j in range(1, gy_n):
        pl.semaphore_signal(barrier, inc=1, device_id=(gx, lax.rem(gy + j, gy_n)), device_id_type=MESH)
    load_fields = pltpu.make_async_copy(fields, field, load_sem.at[0])
    load_fields.start()
    load_flow = pltpu.make_async_copy(vel, flow, load_sem.at[1])
    load_flow.start()
    c = idx[...]
    zrow = c % 128
    xyrow = c // 128
    bhot[...] = jnp.where(lax.broadcasted_iota(jnp.int32, (256, 4096), 0) == xyrow, 1.0, 0.0).astype(BF)
    pl.semaphore_wait(barrier, gx_n + gy_n - 2)
    for j in range(1, gy_n):
        pl.semaphore_signal(word, inc=1, device_id=(gx, lax.rem(gy + j, gy_n)), device_id_type=MESH)
    swap = pltpu.make_async_remote_copy(
        src_ref=shares.at[1], dst_ref=theirs, send_sem=swap_sem.at[0], recv_sem=swap_sem.at[1],
        device_id=(gx, gy + 1 - 2 * lax.rem(gy, 2)), device_id_type=MESH)
    swap.start()
    heat_column = column(heat_release)[:, 0:1]
    swap.wait()
    rates = shares[0].astype(jnp.float32) + theirs[...].astype(jnp.float32)
    heat_row = jnp.sum(rates * heat_column, axis=0, keepdims=True)
    upper = heat_row.astype(BF).astype(jnp.float32)
    rest = heat_row - upper
    for h in range(2):
        part = upper if h == 0 else rest
        ohot[h * 128:(h + 1) * 128, :] = jnp.where(lax.broadcasted_iota(jnp.int32, (128, 4096), 0) == zrow, part, 0.0).astype(BF)
    both = mm(bhot[...], ohot[...], ((1,), (1,)), None)
    src = div[...] - (both[:, :128] + both[:, 128:])
    zt = mm(fz[...], src, ((1,), (1,)))
    sbuf[:, 0, :] = zt[:, :128]
    sbuf[:, 1, :] = zt[:, 128:]

    pl.semaphore_wait(word, gy_n - 1)
    everyone(lambda ta, tb: pltpu.make_async_remote_copy(
        src_ref=sbuf.at[ta * gy_n + tb], dst_ref=rbuf.at[gy, gx], send_sem=send_sem, recv_sem=recv_sem,
        device_id=(ta, tb), device_id_type=MESH).start())
    own = pltpu.make_async_copy(sbuf.at[me], rbuf.at[gy, gx], recv_sem)
    own.start()
    lane = lax.broadcasted_iota(jnp.int32, (8, 128), 1) // 16
    col = lax.broadcasted_iota(jnp.int32, (8, 128), 1)
    mode = lax.broadcasted_iota(jnp.int32, (1, 128), 1)
    lz = jnp.sum(jnp.where(mode == me, lamz[...], 0.0), axis=1, keepdims=True)
    sym = lamx[...] + lamy[...] + lz
    anchor = (lax.broadcasted_iota(jnp.int32, (128, 256), 0) == 0) & (lax.broadcasted_iota(jnp.int32, (128, 256), 1) == 0) & (me == 0)
    g = jnp.where(anchor, 0.0, 1.0 / jnp.where(anchor, 1.0, sym))
    high = c >= 16384
    xh = jnp.where(high, 15 - c // 2048, c // 2048)
    xyh = xh * 16 + xyrow % 16
    kk = jnp.where(high, 128, 0) + zrow
    bhot[...] = jnp.where(lax.broadcasted_iota(jnp.int32, (256, 4096), 0) == kk, 1.0, 0.0).astype(BF)
    half = (rates * 0.5).astype(BF)
    flat = stage.reshape(16 * 24 * 16, 128)

    def react(pair):
        rows = [jnp.where(xyh == pair * 16 + q, half, jnp.zeros_like(half)) for q in range(16)]
        rows = jnp.concatenate(rows, axis=0)
        new = field[pair * 384:(pair + 1) * 384, :] + mm(rows, bhot[...], ((1,), (1,)), None)
        for q in range(16):
            flat[pl.ds(pair * 384 + q, 24, stride=16), :] = new[q * 24:(q + 1) * 24, :128]
            flat[pl.ds((15 - pair) * 384 + q, 24, stride=16), :] = new[q * 24:(q + 1) * 24, 128:]
        for x in (pair, 15 - pair):
            pltpu.make_async_copy(stage.at[x], sout.at[:, x], out_sem.at[x]).start()

    load_fields.wait()
    for pair in range(4):
        react(pair)
    pltpu.make_async_copy(rbuf, rbuf, recv_sem).wait()
    pltpu.make_async_copy(sbuf.at[pl.ds(0, n - 1)], sbuf.at[pl.ds(0, n - 1)], send_sem).wait()

    planes = [[None, None] for _ in range(16)]
    for h in range(2):
        for bh in range(2):
            got = units([rbuf[bh * 8 + b, :, h, :] for b in range(8)], lane)
            for xlo in range(8):
                planes[h * 8 + xlo][bh] = got[xlo]
    plane = jnp.concatenate([jnp.concatenate(p, axis=1) for p in planes], axis=0)
    t = mm(fx[...], plane, ((1,), (0,)))
    t = mm(t, fy[...], ((1,), (1,))) * g
    t = mm(t, fy[...], ((1,), (0,)))
    p = mm(fxt[...], t, ((1,), (0,)))
    px = [[p[x * 8:(x + 1) * 8, bh * 128:(bh + 1) * 128] for bh in range(2)] for x in range(16)]
    before = pltpu.roll(p, 1, 1)
    for bh in range(2):
        edge_x = pltpu.roll(px[15][bh], 1, 0)
        edge_y = before[0:8, bh * 128:(bh + 1) * 128]
        for x in range(1, 16):
            edge_y = jnp.where(col % 16 == x, pltpu.roll(before[x * 8:(x + 1) * 8, bh * 128:(bh + 1) * 128], x, 1), edge_y)
        for h in range(2):
            got = units([px[h * 8 + xlo][bh] for xlo in range(8)], lane)
            for b in range(8):
                tbuf[bh * 8 + b, :, h, :] = got[b]
        for b in range(8):
            ex = edge_x if b == 0 else pltpu.roll(edge_x, 128 - b * 16, 1)
            ey = pltpu.roll(edge_y, (128 - b * 16 + 16) % 128, 1) if b != 1 else edge_y
            tbuf[bh * 8 + b, :, 2, :] = jnp.where(lane == 0, ex, ey)

    everyone(lambda ta, tb: pltpu.make_async_remote_copy(
        src_ref=tbuf.at[tb, ta], dst_ref=pbuf.at[me], send_sem=send_sem2, recv_sem=recv_sem2,
        device_id=(ta, tb), device_id_type=MESH).start())
    own = pltpu.make_async_copy(tbuf.at[gy, gx], pbuf.at[me], recv_sem2)
    own.start()
    for pair in range(4, 8):
        react(pair)
    pltpu.make_async_copy(pbuf, pbuf, recv_sem2).wait()
    pltpu.make_async_copy(pbuf.at[pl.ds(0, n - 1)], pbuf.at[pl.ds(0, n - 1)], send_sem2).wait()
    rows = [mm(pbuf[:, h, :], fz[...], ((0,), (0,))) for h in range(3)]
    q = jnp.concatenate(rows[:2], axis=0)
    west = rows[2][0:16]
    south = rows[2][16:32]
    load_flow.wait()
    out[2] = flow[2] - (q - pltpu.roll(q, 1, 1))
    out[0] = flow[0] - (q - jnp.concatenate([west, q[:240]], axis=0))
    sub = lax.broadcasted_iota(jnp.int32, (16, 128), 0)
    for x in range(16):
        cur = q[x * 16:(x + 1) * 16]
        prev = jnp.where(sub == 0, jnp.broadcast_to(south[x:x + 1], (16, 128)), pltpu.roll(cur, 1, 0))
        out[1, x * 16:(x + 1) * 16] = flow[1, x * 16:(x + 1) * 16] - (cur - prev)

    for x in range(16):
        pltpu.make_async_copy(stage.at[x], sout.at[:, x], out_sem.at[x]).wait()


def finish(fields, shares, div, velocity, heat_release, react_index):
    gx_n, gy_n = lax.axis_size("gx"), lax.axis_size("gy")
    fz, lz = real_basis(128)
    fx, lx = real_basis(128)
    fy, ly = real_basis(256)
    fxp = fx.reshape(128, 8, 16).transpose(0, 2, 1).reshape(128, 128)
    vm = pl.BlockSpec(memory_space=pltpu.VMEM)
    hb = pl.BlockSpec(memory_space=pl.ANY)
    args = (heat_release, fields, shares, react_index.reshape(1, 4096), div, velocity.reshape(3, 256, 128), jnp.asarray(fz), jnp.asarray(fxp), jnp.asarray(np.ascontiguousarray(fxp.T)), jnp.asarray(fy),
            jnp.asarray(lx[:, None]), jnp.asarray(ly[None, :]), jnp.asarray(lz[None, :]))
    species_out, out = pl.pallas_call(
        functools.partial(finish_kernel, gx_n, gy_n),
        out_shape=(jax.ShapeDtypeStruct((24, 16, 16, 128), jnp.float32), jax.ShapeDtypeStruct((3, 256, 128), jnp.float32)),
        in_specs=[pl.BlockSpec(memory_space=pltpu.SMEM), hb, vm, vm, vm, hb] + [vm] * (len(args) - 6), out_specs=(pl.BlockSpec(memory_space=pl.ANY), vm),
        scratch_shapes=[
            pltpu.VMEM((16, 24, 16, 128), jnp.float32), pltpu.VMEM((256, 4096), BF), pltpu.VMEM((256, 4096), BF), pltpu.VMEM((24, 4096), BF),
            pltpu.VMEM((128, 2, 128), jnp.float32), pltpu.VMEM((16, 8, 2, 128), jnp.float32),
            pltpu.VMEM((16, 8, 3, 128), jnp.float32), pltpu.VMEM((128, 3, 128), jnp.float32),
            pltpu.SemaphoreType.DMA, pltpu.SemaphoreType.DMA, pltpu.SemaphoreType.DMA, pltpu.SemaphoreType.DMA,
            pltpu.SemaphoreType.DMA((16,)), pltpu.SemaphoreType.DMA((2,)), pltpu.SemaphoreType.DMA((2,)),
            pltpu.VMEM((3072, 256), jnp.float32), pltpu.VMEM((3, 256, 128), jnp.float32),
            pltpu.SemaphoreType.REGULAR],
        compiler_params=pltpu.CompilerParams(collective_id=1, has_side_effects=True),
        name="finish",
    )(*args)
    return species_out, out.reshape(velocity.shape)


def per_device(species, diffusivity, lewis_number, velocity, layer_one, layer_two, layer_three, layer_four,
               heat_release, react_index, react_count):
    fields, gb, div, notes = transport(species, diffusivity, lewis_number, velocity, react_index, react_count)
    shares = network(notes, gb, layer_one, layer_two, layer_three, layer_four, react_count)
    return finish(fields, shares, div, velocity, heat_release, react_index)


def solution(mesh):
    return jax.shard_map(
        per_device,
        mesh=mesh,
        in_specs=(
            P(None, "gx", "gy", None),
            P("gx", "gy", None),
            P(),
            P(None, "gx", "gy", None),
            P(),
            P(),
            P(),
            P(),
            P(),
            P("gx", "gy", None),
            P("gx", "gy"),
        ),
        out_specs=(P(None, "gx", "gy", None), P(None, "gx", "gy", None)),
        check_vma=False,
    )
```

```python
import functools

import jax
import jax.numpy as jnp
import numpy as np
from jax import lax
from jax.experimental import pallas as pl
from jax.experimental.pallas import tpu as pltpu
from jax.sharding import PartitionSpec as P

MESH = pl.DeviceIdType.MESH
HI = lax.Precision.HIGHEST
BF = jnp.bfloat16
PITCH = 24


def next_along(v):
    return pltpu.roll(v, 127, 1)


def column(ref):
    rows = lax.broadcasted_iota(jnp.int32, (24, 128), 0)
    out = jnp.zeros((24, 128), jnp.float32)
    for s in range(24):
        out = jnp.where(rows == s, ref[s], out)
    return out


def transport_kernel(gx_n, gy_n, lewis, sp, dif, vel_in, idx, cnt, shift, fields, field_pair, div, other,
                     stage, y0, y1, dp, ax, ay, az, sendx, recvx, sendy, recvy, sendc, recvc, sendv, recvv, note,
                     fout, gb, vel, azm, load_sem, ssem, rsem, out_sem):
    gx = lax.axis_index("gx")
    gy = lax.axis_index("gy")
    east, west = lax.rem(gx + 1, gx_n), lax.rem(gx + gx_n - 1, gx_n)
    north, south = lax.rem(gy + 1, gy_n), lax.rem(gy + gy_n - 1, gy_n)
    mate = gy + 1 - 2 * lax.rem(gy, 2)
    diag = ((east, north), (east, south), (west, north), (west, south))
    barrier = pltpu.get_barrier_semaphore()
    for dev in ((east, gy), (west, gy), (gx, north), (gx, south)) + diag:
        pl.semaphore_signal(barrier, inc=1, device_id=dev, device_id_type=MESH)

    def load(x):
        return pltpu.make_async_copy(sp.at[:, x], stage.at[x], load_sem.at[x])

    def start_load(k, carry):
        load(lax.rem(k + 14, 16)).start()
        return carry
    lax.fori_loop(0, 16, start_load, 0)
    load_flow = pltpu.make_async_copy(vel_in, vel, out_sem.at[4])
    load_flow.start()

    flat = stage.reshape(16 * 24 * 16, 128)

    def copy(src, dst, k, dev):
        return pltpu.make_async_remote_copy(src_ref=src, dst_ref=dst, send_sem=ssem.at[k], recv_sem=rsem.at[k],
                                            device_id=dev, device_id_type=MESH)

    copies = [copy(sendx.at[0], recvx.at[0], 0, (east, gy)), copy(sendx.at[1], recvx.at[1], 1, (west, gy)),
              copy(sendy.at[0], recvy.at[0], 2, (gx, north)), copy(sendy.at[1], recvy.at[1], 3, (gx, south)),
              copy(sendc.at[0], recvc.at[0], 4, diag[0]), copy(sendc.at[1], recvc.at[1], 5, diag[1]),
              copy(sendc.at[2], recvc.at[2], 6, diag[2]), copy(sendc.at[3], recvc.at[3], 7, diag[3]),
              copy(sendv.at[0], recvv.at[0], 8, (west, gy)), copy(sendv.at[1], recvv.at[1], 9, (gx, south)),
              copy(gb.at[pl.ds(768, 2304)], field_pair.at[1, pl.ds(768, 2304)], 10, (gx, mate)),
              copy(gb.at[pl.ds(0, 768)], field_pair.at[1, pl.ds(0, 768)], 11, (gx, mate)),
              copy(note.at[0], other.at[1], 12, (gx, mate))]

    def spread(x):
        load(x).wait()
        for y in range(16):
            y0[(x + 2) * 20 + y + 2] = flat[pl.ds(x * 384 + y, 24, stride=16), :]

    def pack_x(k, carry):
        x = lax.rem(k + 14, 16)
        spread(x)
        for y in range(0, 16, 2):
            two = jnp.concatenate([y0[(x + 2) * 20 + y + 2], y0[(x + 2) * 20 + y + 3]], axis=0)
            sendx[k // 2, lax.rem(k, 2), y * 24:y * 24 + 48, :] = two.astype(BF)
        sendx[k // 2, lax.rem(k, 2), 384:400, :] = dif[pl.ds(pl.multiple_of(x * 16, 16), 16), :].astype(BF)
        return carry
    lax.fori_loop(0, 4, pack_x, 0)
    pl.semaphore_wait(barrier, 8)
    copies[0].start()
    copies[1].start()
    load_flow.wait()
    sendv[0] = vel[0, 0:16, :]
    sendv[1] = vel[1, pl.ds(0, 16, stride=16), :]
    copies[8].start()
    copies[9].start()

    def spread_rest(x, carry):
        spread(x)
        return carry
    lax.fori_loop(2, 14, spread_rest, 0)

    def pack_y(k, carry):
        y = lax.rem(k + 14, 16)
        for x in range(0, 16, 2):
            two = jnp.concatenate([y0[(x + 2) * 20 + y + 2], y0[(x + 3) * 20 + y + 2]], axis=0)
            sendy[k // 2, lax.rem(k, 2), x * 24:x * 24 + 48, :] = two.astype(BF)
        sendy[k // 2, lax.rem(k, 2), 384:400, :] = dif[pl.ds(y, 16, stride=16), :].astype(BF)
        return carry
    lax.fori_loop(0, 4, pack_y, 0)
    copies[2].start()
    copies[3].start()
    for k, (x, y) in enumerate(((15, 15), (15, 0), (0, 15), (0, 0))):
        drow = jnp.broadcast_to(dif[x * 16 + y:x * 16 + y + 1, :], (8, 128))
        sendc[k] = jnp.concatenate([y0[(x + 2) * 20 + y + 2], drow], axis=0).astype(BF)
        copies[4 + k].start()
    note[0, 0:1, :] = idx[...].astype(jnp.float32)
    note[0, 1:2, :] = jnp.broadcast_to(cnt[...].astype(jnp.float32), (1, 4096))
    other[0] = note[0]
    copies[12].start()

    for x in range(16):
        dp[pl.ds((x + 2) * PITCH + 2, 16), :] = dif[x * 16:x * 16 + 16, :]

    def conduct():
        d = dp[...]
        ax[...] = 0.5 * (d + jnp.concatenate([d[PITCH:], d[:PITCH]], axis=0))
        ay[...] = 0.5 * (d + pltpu.roll(d, 20 * PITCH - 1, 0))
        up = 0.5 * (d + next_along(d))
        az[...] = up
        azm[...] = pltpu.roll(up, 1, 1)
    conduct()
    scale = 0.03 / column(lewis)

    def row(ref, r):
        return ref[pl.ds(r, 24, stride=0), :]

    def line(src, i, js):
        c = src[i * 20 + js[0]]
        if len(js) > 2:
            block = src[pl.ds(i * 20 + js[0], len(js))].reshape(len(js) * 24, 128)
            upper = block.astype(BF)
            rest = (block - upper.astype(jnp.float32)).astype(BF)
            dz = jnp.dot(jnp.concatenate([upper, rest], axis=1), shift[...], preferred_element_type=jnp.float32)
        back = row(ay, i * PITCH + js[0] - 1) * (c - src[i * 20 + js[0] - 1])
        for j in js:
            r = i * PITCH + j
            after = src[i * 20 + j + 1]
            ahead = row(ay, r) * (after - c)
            fx = row(ax, r) * (src[i * 20 + j + 20] - c) - row(ax, r - PITCH) * (c - src[i * 20 + j - 20])
            if len(js) > 2:
                at = (j - js[0]) * 24
                fz = row(az, r) * dz[at:at + 24, :128] - row(azm, r) * dz[at:at + 24, 128:]
            else:
                t = row(az, r) * (next_along(c) - c)
                fz = t - pltpu.roll(t, 1, 1)
            yield c + scale * (fx + (ahead - back) + fz)
            c, back = after, ahead

    def first(n, start, stride, *runs):
        def body(k, carry):
            i = start + stride * k
            for js in runs:
                for j, v in zip(js, line(y0, i, js)):
                    y1[i * 20 + j] = v
            return carry
        lax.fori_loop(0, n, body, 0)

    def second(lo, hi):
        def body(pair, carry):
            js = range(2, 18)
            kept = None
            for j, low, high in zip(js, line(y1, pair + 2, js), line(y1, 17 - pair, js)):
                val = jnp.concatenate([low, high], axis=1)
                base = pl.multiple_of(pair * 384 + (j - 2) * 24, 8)
                fout[pl.ds(base, 24), :] = val
                if j % 2 == 0:
                    kept = val
                else:
                    gb[pl.ds(pl.multiple_of(pair * 384 + (j - 3) * 24, 16), 48), :] = jnp.concatenate([kept, val], axis=0).astype(BF)
            return carry
        lax.fori_loop(lo, hi, body, 0)

    first(14, 3, 1, range(3, 17))
    for k in (2, 3):
        copies[k].wait_recv()

    def unpack_y(k, carry):
        d, p = k // 2, lax.rem(k, 2)
        j = p + 18 * d
        for x in range(0, 16, 2):
            two = recvy[d, p, x * 24:x * 24 + 48, :].astype(jnp.float32)
            y0[(x + 2) * 20 + j] = two[:24]
            y0[(x + 3) * 20 + j] = two[24:]
        drows = recvy[d, p, 384:400, :].astype(jnp.float32)
        for x in range(16):
            dp[pl.ds((x + 2) * PITCH + j, 1), :] = drows[x:x + 1]
        return carry
    lax.fori_loop(0, 4, unpack_y, 0)
    conduct()
    first(14, 3, 1, range(1, 3), range(17, 19))
    second(2, 8)
    copies[10].start()
    stores = [pltpu.make_async_copy(gb.at[pl.ds(768, 2304)], field_pair.at[0, pl.ds(768, 2304)], out_sem.at[0]),
              pltpu.make_async_copy(fout.at[pl.ds(768, 2304)], fields.at[pl.ds(768, 2304)], out_sem.at[1]),
              pltpu.make_async_copy(gb.at[pl.ds(0, 768)], field_pair.at[0, pl.ds(0, 768)], out_sem.at[2]),
              pltpu.make_async_copy(fout.at[pl.ds(0, 768)], fields.at[pl.ds(0, 768)], out_sem.at[3])]
    stores[0].start()
    stores[1].start()
    for k in (0, 1, 4, 5, 6, 7, 8, 9):
        copies[k].wait_recv()

    def unpack_x(k, carry):
        d, p = k // 2, lax.rem(k, 2)
        i = p + 18 * d
        for y in range(0, 16, 2):
            two = recvx[d, p, y * 24:y * 24 + 48, :].astype(jnp.float32)
            y0[i * 20 + y + 2] = two[:24]
            y0[i * 20 + y + 3] = two[24:]
        dp[pl.ds(i * PITCH + 2, 16), :] = recvx[d, p, 384:400, :].astype(jnp.float32)
        return carry
    lax.fori_loop(0, 4, unpack_x, 0)
    for k, (i, j) in enumerate(((1, 1), (1, 18), (18, 1), (18, 18))):
        val = recvc[k].astype(jnp.float32)
        y0[i * 20 + j] = val[:24]
        dp[pl.ds(i * PITCH + j, 1), :] = val[24:25]
    conduct()
    first(2, 1, 17, range(2, 18))
    first(2, 2, 15, range(1, 19))
    second(0, 2)
    copies[11].start()
    stores[2].start()
    stores[3].start()

    sub = lax.broadcasted_iota(jnp.int32, (16, 128), 0)
    for x in range(16):
        here = slice(x * 16, x * 16 + 16)
        nx = recvv[0] if x == 15 else vel[0, x * 16 + 16:x * 16 + 32, :]
        uy = vel[1, here, :]
        ny = jnp.where(sub == 15, jnp.broadcast_to(recvv[1, x:x + 1, :], (16, 128)), pltpu.roll(uy, 15, 0))
        uz = vel[2, here, :]
        div[here, :] = (nx - vel[0, here, :]) + (ny - uy) + (next_along(uz) - uz)
    for k in (10, 11, 12):
        copies[k].wait_recv()
    for c in copies:
        c.wait_send()
    for c in stores:
        c.wait()


def transport(species, diffusivity, lewis_number, velocity, react_index, react_count):
    gx_n, gy_n = lax.axis_size("gx"), lax.axis_size("gy")
    vm = pl.BlockSpec(memory_space=pltpu.VMEM)
    hb = pl.BlockSpec(memory_space=pl.ANY)
    sm = pl.BlockSpec(memory_space=pltpu.SMEM)
    f32 = jnp.float32
    ahead = np.roll(np.eye(128), 1, 0) - np.eye(128)
    behind = np.eye(128) - np.roll(np.eye(128), -1, 0)
    shift = np.tile(np.concatenate([ahead, behind], axis=1), (2, 1))
    return pl.pallas_call(
        functools.partial(transport_kernel, gx_n, gy_n),
        out_shape=(jax.ShapeDtypeStruct((3072, 256), f32), jax.ShapeDtypeStruct((2, 3072, 256), BF),
                   jax.ShapeDtypeStruct((256, 128), f32), jax.ShapeDtypeStruct((2, 2, 4096), f32)),
        in_specs=[sm, hb, vm, hb, vm, vm, vm], out_specs=(hb, hb, vm, vm),
        scratch_shapes=[
            pltpu.VMEM((16, 24, 16, 128), f32), pltpu.VMEM((400, 24, 128), f32), pltpu.VMEM((400, 24, 128), f32),
            pltpu.VMEM((20 * PITCH, 128), f32), pltpu.VMEM((20 * PITCH, 128), f32), pltpu.VMEM((20 * PITCH, 128), f32),
            pltpu.VMEM((20 * PITCH, 128), f32),
            pltpu.VMEM((2, 2, 400, 128), BF), pltpu.VMEM((2, 2, 400, 128), BF),
            pltpu.VMEM((2, 2, 400, 128), BF), pltpu.VMEM((2, 2, 400, 128), BF),
            pltpu.VMEM((4, 32, 128), BF), pltpu.VMEM((4, 32, 128), BF),
            pltpu.VMEM((2, 16, 128), f32), pltpu.VMEM((2, 16, 128), f32), pltpu.VMEM((1, 2, 4096), f32),
            pltpu.VMEM((3072, 256), f32), pltpu.VMEM((3072, 256), BF), pltpu.VMEM((3, 256, 128), f32), pltpu.VMEM((20 * PITCH, 128), f32),
            pltpu.SemaphoreType.DMA((16,)), pltpu.SemaphoreType.DMA((13,)), pltpu.SemaphoreType.DMA((13,)),
            pltpu.SemaphoreType.DMA((5,))],
        compiler_params=pltpu.CompilerParams(collective_id=2, has_side_effects=True),
        name="transport",
    )(lewis_number, species, diffusivity.reshape(256, 128), velocity.reshape(3, 256, 128), react_index.reshape(1, 4096), react_count, jnp.asarray(shift, BF))


def silu(v):
    half = 0.5 * v
    return (half + half * jnp.tanh(half)).astype(BF)


def network_kernel(count, notes_in, gb_in, w1t_in, w2_in, w3_in, w4_in, out, notes, gb, w1t, w2, w3, w4, w1, rows, sem):
    pairs = ((notes_in, notes), (gb_in.at[0], gb.at[0]), (gb_in.at[1], gb.at[1]), (w1t_in, w1t), (w2_in, w2),
             (w3_in, w3), (w4_in, w4))
    loads = [pltpu.make_async_copy(a, b, sem.at[i]) for i, (a, b) in enumerate(pairs)]
    for c in loads:
        c.start()
    out[...] = jnp.zeros_like(out)
    loads[0].wait()
    mine = count[0, 0]
    theirs = jnp.max(notes[1, 1:2, 0:128]).astype(jnp.int32)
    own = ((mine + 255) // 256 + 1) // 2
    units = own + (theirs + 255) // 256 // 2
    slot = lax.broadcasted_iota(jnp.int32, (24, 256), 1)
    rows256 = lax.broadcasted_iota(jnp.int32, (256, 256), 0)

    def dot(w, v):
        return jnp.dot(w[...], v, preferred_element_type=jnp.float32)

    def place(t):
        t = jnp.minimum(t, units - 1)
        which = (t >= own).astype(jnp.int32)
        unit = jnp.where(t >= own, 2 * (t - own) + 1, 2 * t)
        return which, unit, pl.ds(pl.multiple_of(unit * 256, 256), 256)

    def gather(t):
        which, _, where = place(t)
        c = notes[which, 0:1, where].astype(jnp.int32)
        x = c // 2048
        high = x >= 8
        xyh = jnp.where(high, 15 - x, x) * 16 + (c // 128) % 16
        kk = jnp.where(high, 128, 0) + c % 128
        pick = jnp.where(rows256 == kk, 1.0, 0.0).astype(BF)
        acc = jnp.zeros((24, 256), jnp.float32)
        for part in range(2):
            t = dot(gb.at[which, part * 1536:(part + 1) * 1536, :], pick)
            for q in range(64):
                acc = acc + jnp.where(xyh == part * 64 + q, t[q * 24:(q + 1) * 24], 0.0)
        return acc.astype(BF)

    loads[1].wait()
    loads[2].wait()
    for k in range(2):
        rows[k] = gather(k)
    for c in loads[3:]:
        c.wait()
    w1[...] = jnp.transpose(w1t[...].astype(jnp.float32)).astype(BF)

    def body(it, carry):
        hs = [rows[k] for k in range(2)]
        hs = [silu(dot(w1, h)) for h in hs]
        hs = [silu(dot(w2, h)) for h in hs]
        later = [gather(2 * it + 2 + k) for k in range(2)]
        hs = [silu(dot(w3, h)) for h in hs]
        for k, h in enumerate(hs):
            which, unit, where = place(2 * it + k)
            limit = jnp.where(which == 0, mine, theirs)
            out[which, :, where] = jnp.where(slot + unit * 256 < limit, dot(w4, h), 0.0).astype(BF)
            rows[k] = later[k]
        return carry
    lax.fori_loop(0, (units + 1) // 2, body, 0)


def network(notes, gb, w1, w2, w3, w4, count):
    hb = pl.BlockSpec(memory_space=pl.ANY)
    args = (notes, gb, w1.T, w2, w3, w4)
    return pl.pallas_call(
        network_kernel,
        out_shape=jax.ShapeDtypeStruct((2, 24, 4096), BF),
        in_specs=[pl.BlockSpec(memory_space=pltpu.SMEM)] + [hb] * 6,
        out_specs=pl.BlockSpec(memory_space=pltpu.VMEM),
        scratch_shapes=[pltpu.VMEM(a.shape, a.dtype) for a in args]
        + [pltpu.VMEM((1600, 24), BF), pltpu.VMEM((2, 24, 256), BF), pltpu.SemaphoreType.DMA((7,))],
        name="network",
    )(count, *args)


def real_basis(n):
    k = np.arange(n)
    j = np.arange(n)
    wave = np.where(k <= n // 2, k, k - n // 2)
    ang = 2.0 * np.pi * ((wave[:, None] * j[None, :]) % n) / n
    rows = np.where((k <= n // 2)[:, None], np.cos(ang), np.sin(ang)) * np.sqrt(2.0 / n)
    rows[0] *= np.sqrt(0.5)
    rows[n // 2] *= np.sqrt(0.5)
    lam = 2.0 * np.cos(2.0 * np.pi * wave / n) - 2.0
    return rows.astype(np.float32), lam.astype(np.float32)


def mm(a, b, dims, precision=HI):
    return lax.dot_general(a, b, (dims, ((), ())), precision=precision, preferred_element_type=jnp.float32)


def units(grid, lane):
    turned = []
    for d in range(8):
        w = grid[d]
        for u in range(1, 8):
            w = jnp.where(lane == u, grid[(u + d) % 8], w)
        turned.append(w if d == 0 else pltpu.roll(w, d * 16, 1))
    out = []
    for v in range(8):
        acc = turned[(0 - v) % 8]
        for u in range(1, 8):
            acc = jnp.where(lane == u, turned[(u - v) % 8], acc)
        out.append(acc)
    return out


def finish_kernel(gx_n, gy_n, heat_release, fields, shares_in, idx_in, div_in, vel, fz_in, fx_in, fxt_in, fy_in, lamx_in, lamy_in, lamz_in, sout, out,
                  stage, ohot, bhot, theirs, sbuf, rbuf, tbuf, pbuf, send_sem, recv_sem, send_sem2, recv_sem2, out_sem, swap_sem, load_sem, field, flow, word,
                  shares, idx, div, fz, fx, fxt, fy, lamx, lamy, lamz):
    gx = lax.axis_index("gx")
    gy = lax.axis_index("gy")
    n = gx_n * gy_n
    me = gx * gy_n + gy
    barrier = pltpu.get_barrier_semaphore()

    def everyone(act):
        def rows_of(i, carry):
            ta = lax.rem(gx + i, gx_n)
            for j in range(gy_n):
                act(ta, lax.rem(gy + j, gy_n))
            return carry
        lax.fori_loop(1, gx_n, rows_of, 0)
        for j in range(1, gy_n):
            act(gx, lax.rem(gy + j, gy_n))

    for j in range(1, gx_n):
        pl.semaphore_signal(barrier, inc=1, device_id=(lax.rem(gx + j, gx_n), gy), device_id_type=MESH)
    for j in range(1, gy_n):
        pl.semaphore_signal(barrier, inc=1, device_id=(gx, lax.rem(gy + j, gy_n)), device_id_type=MESH)
    pairs = ((idx_in, idx), (shares_in, shares), (div_in, div), (fz_in, fz), (fx_in, fx), (fxt_in, fxt), (fy_in, fy),
             (lamx_in, lamx), (lamy_in, lamy), (lamz_in, lamz), (fields, field), (vel, flow))
    loads = [pltpu.make_async_copy(a, b, load_sem.at[i]) for i, (a, b) in enumerate(pairs)]
    for c in loads:
        c.start()
    loads[0].wait()
    c = idx[...]
    zrow = c % 128
    xyrow = c // 128
    bhot[...] = jnp.where(lax.broadcasted_iota(jnp.int32, (256, 4096), 0) == xyrow, 1.0, 0.0).astype(BF)
    loads[1].wait()
    pl.semaphore_wait(barrier, gx_n + gy_n - 2)
    for j in range(1, gy_n):
        pl.semaphore_signal(word, inc=1, device_id=(gx, lax.rem(gy + j, gy_n)), device_id_type=MESH)
    swap = pltpu.make_async_remote_copy(
        src_ref=shares.at[1], dst_ref=theirs, send_sem=swap_sem.at[0], recv_sem=swap_sem.at[1],
        device_id=(gx, gy + 1 - 2 * lax.rem(gy, 2)), device_id_type=MESH)
    swap.start()
    heat_column = column(heat_release)[:, 0:1]
    swap.wait()
    rates = shares[0].astype(jnp.float32) + theirs[...].astype(jnp.float32)
    heat_row = jnp.sum(rates * heat_column, axis=0, keepdims=True)
    upper = heat_row.astype(BF).astype(jnp.float32)
    rest = heat_row - upper
    for h in range(2):
        part = upper if h == 0 else rest
        ohot[h * 128:(h + 1) * 128, :] = jnp.where(lax.broadcasted_iota(jnp.int32, (128, 4096), 0) == zrow, part, 0.0).astype(BF)
    both = mm(bhot[...], ohot[...], ((1,), (1,)), None)
    loads[2].wait()
    loads[3].wait()
    src = div[...] - (both[:, :128] + both[:, 128:])
    zt = mm(fz[...], src, ((1,), (1,)))
    sbuf[:, 0, :] = zt[:, :128]
    sbuf[:, 1, :] = zt[:, 128:]

    pl.semaphore_wait(word, gy_n - 1)
    everyone(lambda ta, tb: pltpu.make_async_remote_copy(
        src_ref=sbuf.at[ta * gy_n + tb], dst_ref=rbuf.at[gy, gx], send_sem=send_sem, recv_sem=recv_sem,
        device_id=(ta, tb), device_id_type=MESH).start())
    own = pltpu.make_async_copy(sbuf.at[me], rbuf.at[gy, gx], recv_sem)
    own.start()
    for arriving in loads[4:10]:
        arriving.wait()
    lane = lax.broadcasted_iota(jnp.int32, (8, 128), 1) // 16
    col = lax.broadcasted_iota(jnp.int32, (8, 128), 1)
    mode = lax.broadcasted_iota(jnp.int32, (1, 128), 1)
    lz = jnp.sum(jnp.where(mode == me, lamz[...], 0.0), axis=1, keepdims=True)
    sym = lamx[...] + lamy[...] + lz
    anchor = (lax.broadcasted_iota(jnp.int32, (128, 256), 0) == 0) & (lax.broadcasted_iota(jnp.int32, (128, 256), 1) == 0) & (me == 0)
    g = jnp.where(anchor, 0.0, 1.0 / jnp.where(anchor, 1.0, sym))
    high = c >= 16384
    xh = jnp.where(high, 15 - c // 2048, c // 2048)
    xyh = xh * 16 + xyrow % 16
    kk = jnp.where(high, 128, 0) + zrow
    bhot[...] = jnp.where(lax.broadcasted_iota(jnp.int32, (256, 4096), 0) == kk, 1.0, 0.0).astype(BF)
    half = (rates * 0.5).astype(BF)
    flat = stage.reshape(16 * 24 * 16, 128)

    def react(pair):
        rows = [jnp.where(xyh == pair * 16 + q, half, jnp.zeros_like(half)) for q in range(16)]
        rows = jnp.concatenate(rows, axis=0)
        new = field[pair * 384:(pair + 1) * 384, :] + mm(rows, bhot[...], ((1,), (1,)), None)
        for q in range(16):
            flat[pl.ds(pair * 384 + q, 24, stride=16), :] = new[q * 24:(q + 1) * 24, :128]
            flat[pl.ds((15 - pair) * 384 + q, 24, stride=16), :] = new[q * 24:(q + 1) * 24, 128:]
        for x in (pair, 15 - pair):
            pltpu.make_async_copy(stage.at[x], sout.at[:, x], out_sem.at[x]).start()

    loads[10].wait()
    for pair in range(4):
        react(pair)
    pltpu.make_async_copy(rbuf, rbuf, recv_sem).wait()
    pltpu.make_async_copy(sbuf.at[pl.ds(0, n - 1)], sbuf.at[pl.ds(0, n - 1)], send_sem).wait()

    planes = [[None, None] for _ in range(16)]
    for h in range(2):
        for bh in range(2):
            got = units([rbuf[bh * 8 + b, :, h, :] for b in range(8)], lane)
            for xlo in range(8):
                planes[h * 8 + xlo][bh] = got[xlo]
    plane = jnp.concatenate([jnp.concatenate(p, axis=1) for p in planes], axis=0)
    t = mm(fx[...], plane, ((1,), (0,)))
    t = mm(t, fy[...], ((1,), (1,))) * g
    t = mm(t, fy[...], ((1,), (0,)))
    p = mm(fxt[...], t, ((1,), (0,)))
    px = [[p[x * 8:(x + 1) * 8, bh * 128:(bh + 1) * 128] for bh in range(2)] for x in range(16)]
    before = pltpu.roll(p, 1, 1)
    for bh in range(2):
        edge_x = pltpu.roll(px[15][bh], 1, 0)
        edge_y = before[0:8, bh * 128:(bh + 1) * 128]
        for x in range(1, 16):
            edge_y = jnp.where(col % 16 == x, pltpu.roll(before[x * 8:(x + 1) * 8, bh * 128:(bh + 1) * 128], x, 1), edge_y)
        for h in range(2):
            got = units([px[h * 8 + xlo][bh] for xlo in range(8)], lane)
            for b in range(8):
                tbuf[bh * 8 + b, :, h, :] = got[b]
        for b in range(8):
            ex = edge_x if b == 0 else pltpu.roll(edge_x, 128 - b * 16, 1)
            ey = pltpu.roll(edge_y, (128 - b * 16 + 16) % 128, 1) if b != 1 else edge_y
            tbuf[bh * 8 + b, :, 2, :] = jnp.where(lane == 0, ex, ey)

    everyone(lambda ta, tb: pltpu.make_async_remote_copy(
        src_ref=tbuf.at[tb, ta], dst_ref=pbuf.at[me], send_sem=send_sem2, recv_sem=recv_sem2,
        device_id=(ta, tb), device_id_type=MESH).start())
    own = pltpu.make_async_copy(tbuf.at[gy, gx], pbuf.at[me], recv_sem2)
    own.start()
    for pair in range(4, 8):
        react(pair)
    pltpu.make_async_copy(pbuf, pbuf, recv_sem2).wait()
    pltpu.make_async_copy(pbuf.at[pl.ds(0, n - 1)], pbuf.at[pl.ds(0, n - 1)], send_sem2).wait()
    rows = [mm(pbuf[:, h, :], fz[...], ((0,), (0,))) for h in range(3)]
    q = jnp.concatenate(rows[:2], axis=0)
    west = rows[2][0:16]
    south = rows[2][16:32]
    loads[11].wait()
    out[2] = flow[2] - (q - pltpu.roll(q, 1, 1))
    out[0] = flow[0] - (q - jnp.concatenate([west, q[:240]], axis=0))
    sub = lax.broadcasted_iota(jnp.int32, (16, 128), 0)
    for x in range(16):
        cur = q[x * 16:(x + 1) * 16]
        prev = jnp.where(sub == 0, jnp.broadcast_to(south[x:x + 1], (16, 128)), pltpu.roll(cur, 1, 0))
        out[1, x * 16:(x + 1) * 16] = flow[1, x * 16:(x + 1) * 16] - (cur - prev)

    for x in range(16):
        pltpu.make_async_copy(stage.at[x], sout.at[:, x], out_sem.at[x]).wait()


def finish(fields, shares, div, velocity, heat_release, react_index):
    gx_n, gy_n = lax.axis_size("gx"), lax.axis_size("gy")
    fz, lz = real_basis(128)
    fx, lx = real_basis(128)
    fy, ly = real_basis(256)
    fxp = fx.reshape(128, 8, 16).transpose(0, 2, 1).reshape(128, 128)
    vm = pl.BlockSpec(memory_space=pltpu.VMEM)
    hb = pl.BlockSpec(memory_space=pl.ANY)
    args = (heat_release, fields, shares, react_index.reshape(1, 4096), div, velocity.reshape(3, 256, 128), jnp.asarray(fz), jnp.asarray(fxp), jnp.asarray(np.ascontiguousarray(fxp.T)), jnp.asarray(fy),
            jnp.asarray(lx[:, None]), jnp.asarray(ly[None, :]), jnp.asarray(lz[None, :]))
    species_out, out = pl.pallas_call(
        functools.partial(finish_kernel, gx_n, gy_n),
        out_shape=(jax.ShapeDtypeStruct((24, 16, 16, 128), jnp.float32), jax.ShapeDtypeStruct((3, 256, 128), jnp.float32)),
        in_specs=[pl.BlockSpec(memory_space=pltpu.SMEM), hb] + [hb] * (len(args) - 2), out_specs=(pl.BlockSpec(memory_space=pl.ANY), vm),
        scratch_shapes=[
            pltpu.VMEM((16, 24, 16, 128), jnp.float32), pltpu.VMEM((256, 4096), BF), pltpu.VMEM((256, 4096), BF), pltpu.VMEM((24, 4096), BF),
            pltpu.VMEM((128, 2, 128), jnp.float32), pltpu.VMEM((16, 8, 2, 128), jnp.float32),
            pltpu.VMEM((16, 8, 3, 128), jnp.float32), pltpu.VMEM((128, 3, 128), jnp.float32),
            pltpu.SemaphoreType.DMA, pltpu.SemaphoreType.DMA, pltpu.SemaphoreType.DMA, pltpu.SemaphoreType.DMA,
            pltpu.SemaphoreType.DMA((16,)), pltpu.SemaphoreType.DMA((2,)), pltpu.SemaphoreType.DMA((12,)),
            pltpu.VMEM((3072, 256), jnp.float32), pltpu.VMEM((3, 256, 128), jnp.float32),
            pltpu.SemaphoreType.REGULAR] + [pltpu.VMEM(a.shape, a.dtype) for a in (args[2:5] + args[6:])],
        compiler_params=pltpu.CompilerParams(collective_id=1, has_side_effects=True),
        name="finish",
    )(*args)
    species_out, out = hand_over(species_out, out)
    return species_out, out.reshape(velocity.shape)


def hand_over_kernel(species, velocity, species_out, velocity_out, held, flow, in_sem, out_sem):
    loads = [pltpu.make_async_copy(species.at[pl.ds(3 * k, 3)], held.at[pl.ds(3 * k, 3)], in_sem.at[k]) for k in range(8)]
    loads.append(pltpu.make_async_copy(velocity, flow, in_sem.at[8]))
    stores = [pltpu.make_async_copy(held.at[pl.ds(3 * k, 3)], species_out.at[pl.ds(3 * k, 3)], out_sem.at[k]) for k in range(8)]
    stores.append(pltpu.make_async_copy(flow, velocity_out, out_sem.at[8]))
    for c in loads:
        c.start()
    for a, b in zip(loads, stores):
        a.wait()
        b.start()
    for c in stores:
        c.wait()


def hand_over(species, velocity):
    hb = pl.BlockSpec(memory_space=pl.ANY)
    return pl.pallas_call(
        hand_over_kernel,
        out_shape=(jax.ShapeDtypeStruct(species.shape, species.dtype), jax.ShapeDtypeStruct(velocity.shape, velocity.dtype)),
        in_specs=[hb, hb], out_specs=(hb, hb),
        scratch_shapes=[pltpu.VMEM(species.shape, species.dtype), pltpu.VMEM(velocity.shape, velocity.dtype),
                        pltpu.SemaphoreType.DMA((9,)), pltpu.SemaphoreType.DMA((9,))],
        name="hand_over",
    )(species, velocity)


def per_device(species, diffusivity, lewis_number, velocity, layer_one, layer_two, layer_three, layer_four,
               heat_release, react_index, react_count):
    fields, gb, div, notes = transport(species, diffusivity, lewis_number, velocity, react_index, react_count)
    shares = network(notes, gb, layer_one, layer_two, layer_three, layer_four, react_count)
    return finish(fields, shares, div, velocity, heat_release, react_index)


def solution(mesh):
    return jax.shard_map(
        per_device,
        mesh=mesh,
        in_specs=(
            P(None, "gx", "gy", None),
            P("gx", "gy", None),
            P(),
            P(None, "gx", "gy", None),
            P(),
            P(),
            P(),
            P(),
            P(),
            P("gx", "gy", None),
            P("gx", "gy"),
        ),
        out_specs=(P(None, "gx", "gy", None), P(None, "gx", "gy", None)),
        check_vma=False,
    )
```
